32 devices in a mesh: dp: 1 (over z), ep: 32 (over y, x, core).
Axes of the slice: x: 4, y: 4, z: 1, core: 2. Of those that a mesh axis runs over, the one named last changes fastest.
The devices are a block of a 4x4x8 slice.
Arguments:
- x_in: bfloat16 [32768, 1024], P(('dp', 'ep'))
- expert_ids: int32 [32768, 8], P(('dp', 'ep'))
- norm_weight: bfloat16 [1024], replicated
- router_w: bfloat16 [1024, 32], replicated
- router_b: bfloat16 [32], replicated
- w_gate_up: bfloat16 [32, 1024, 1024], P('ep')
- b_gate_up: bfloat16 [32, 1024], P('ep')
- w_down: bfloat16 [32, 512, 1024], P('ep')
- b_down: bfloat16 [32, 1024], P('ep')
Outputs:
- output: bfloat16 [32768, 1024], P(('dp', 'ep'))
All inputs are finite; a program needn't handle non-finite values.
Results may differ from the reference program's by a relative error of at most 0.00637158.
Values are sent between devices in bfloat16 or wider.
A program may use at most 768 MiB of HBM per device.

```python
import jax
import jax.numpy as jnp
from jax import lax

D_MODEL = 1024
D_FF = 512
EXPERTS = 32
TOP_K = 8
TOK_DEV = 1024
GROUP_SIZE = 32

TOKENS = TOK_DEV * GROUP_SIZE
CAPACITY = 4 * TOP_K * TOK_DEV // EXPERTS
HOT_COUNT = EXPERTS // 8
EPSILON = 1e-5
LIMIT = 7.0
ALPHA = 1.702


def draw_routes(key):
    key_hot, key_src = jax.random.split(key)
    expert_order = jax.random.permutation(key_hot, EXPERTS)
    cold_total = TOP_K * TOK_DEV - HOT_COUNT * CAPACITY
    cold_count = EXPERTS - HOT_COUNT
    position = jnp.arange(EXPERTS)
    extra = (position - HOT_COUNT < cold_total % cold_count).astype(jnp.int32)
    counts = jnp.where(position < HOT_COUNT, CAPACITY, cold_total // cold_count + extra)
    ends = jnp.cumsum(counts)
    slot_rank = jnp.sum(jnp.arange(TOP_K * TOK_DEV)[:, None] >= ends[None, :], axis=1)

    def one_source(src_key):
        key_cold, key_tok = jax.random.split(src_key)
        cold = jax.random.permutation(key_cold, expert_order[HOT_COUNT:])
        order = jnp.concatenate([expert_order[:HOT_COUNT], cold])
        table = order[slot_rank].reshape(TOP_K, TOK_DEV).T
        return table[jax.random.permutation(key_tok, TOK_DEV)]

    tables = jax.vmap(one_source)(jax.random.split(key_src, GROUP_SIZE))
    return tables.reshape(TOKENS, TOP_K).astype(jnp.int32)


def stacked_normal(key, shape, scale):
    def one_expert(expert_key):
        return (jax.random.normal(expert_key, shape, jnp.float32) * scale).astype(jnp.bfloat16)
    return lax.map(one_expert, jax.random.split(key, EXPERTS))


def setup_inputs(seed: int = 0, part: int = 0) -> dict:
    shared = jax.random.split(jax.random.key(seed), 7)
    own = jax.random.split(jax.random.fold_in(jax.random.key(seed + 1), part), 2)
    x_in = jax.random.normal(own[0], (TOKENS, D_MODEL), jnp.float32).astype(jnp.bfloat16)
    expert_ids = draw_routes(own[1])
    norm_weight = (1.0 + 0.3 * jax.random.normal(shared[0], (D_MODEL,), jnp.float32)).astype(jnp.bfloat16)
    router_w = (jax.random.normal(shared[1], (D_MODEL, EXPERTS), jnp.float32) * D_MODEL ** -0.5).astype(jnp.bfloat16)
    router_b = (0.7 * jax.random.normal(shared[2], (EXPERTS,), jnp.float32)).astype(jnp.bfloat16)
    w_gate_up = stacked_normal(shared[3], (D_MODEL, 2 * D_FF), 5.0 * D_MODEL ** -0.5)
    b_gate_up = jax.random.normal(shared[4], (EXPERTS, 2 * D_FF), jnp.float32).astype(jnp.bfloat16)
    w_down = stacked_normal(shared[5], (D_FF, D_MODEL), 0.125 * D_FF ** -0.5)
    b_down = (0.5 * jax.random.normal(shared[6], (EXPERTS, D_MODEL), jnp.float32)).astype(jnp.bfloat16)
    return dict(x_in=x_in, expert_ids=expert_ids, norm_weight=norm_weight, router_w=router_w, router_b=router_b, w_gate_up=w_gate_up, b_gate_up=b_gate_up, w_down=w_down, b_down=b_down)


def clamped_glu(gate_up):
    gate = jnp.minimum(gate_up[..., 0::2].astype(jnp.float32), LIMIT)
    linear = jnp.clip(gate_up[..., 1::2].astype(jnp.float32), -LIMIT, LIMIT)
    return (gate * jax.nn.sigmoid(ALPHA * gate) * (linear + 1.0)).astype(jnp.bfloat16)


def reference(x_in, expert_ids, norm_weight, router_w, router_b, w_gate_up, b_gate_up, w_down, b_down):
    x_float = x_in.astype(jnp.float32)
    inv_rms = lax.rsqrt(jnp.mean(x_float * x_float, axis=-1, keepdims=True) + EPSILON)
    hidden = (x_float * inv_rms * norm_weight.astype(jnp.float32)).astype(jnp.bfloat16)
    logits = jnp.dot(hidden, router_w, preferred_element_type=jnp.float32) + router_b.astype(jnp.float32)
    gates = jax.nn.softmax(jnp.take_along_axis(logits, expert_ids, axis=1), axis=-1)
    flat_ids = expert_ids.reshape(-1)
    flat_gates = gates.reshape(-1)
    max_rows = GROUP_SIZE * CAPACITY

    def one_expert(combined, weights):
        expert, gate_up_w, gate_up_b, down_w, down_b = weights
        chosen = flat_ids == expert
        picks = jnp.nonzero(chosen, size=max_rows, fill_value=0)[0]
        valid = jnp.arange(max_rows) < jnp.sum(chosen)
        row_token = picks // TOP_K
        rows = hidden[row_token]
        gate_up = (jnp.dot(rows, gate_up_w, preferred_element_type=jnp.float32) + gate_up_b.astype(jnp.float32)).astype(jnp.bfloat16)
        glu_out = clamped_glu(gate_up)
        expert_out = (jnp.dot(glu_out, down_w, preferred_element_type=jnp.float32) + down_b.astype(jnp.float32)).astype(jnp.bfloat16)
        scale = jnp.where(valid, flat_gates[picks], 0.0)
        combined = combined.at[row_token].add(scale[:, None] * expert_out.astype(jnp.float32))
        return combined, None

    start_sum = jnp.zeros((TOKENS, D_MODEL), jnp.float32)
    combined, _ = lax.scan(one_expert, start_sum, (jnp.arange(EXPERTS, dtype=jnp.int32), w_gate_up, b_gate_up, w_down, b_down))
    return (x_float + combined).astype(jnp.bfloat16)
```

```python
import functools
import math

import jax
import jax.numpy as jnp
from jax import lax
from jax.experimental import pallas as pl
from jax.experimental.pallas import tpu as pltpu
from jax.sharding import PartitionSpec as P

EPSILON = 1e-5
LIMIT = 7.0
ALPHA = 1.702
F32, BF16 = jnp.float32, jnp.bfloat16
MESH = pl.DeviceIdType.MESH
COLS = 256
RING = 4
ORDER = [(0, 0), (0, 3), (0, 1), (1, 0), (0, 2), (1, 3), (1, 1), (1, 2)]
SLOTS = 2 * len(ORDER)


def kernel(x_hbm, ids_v, norm_v, rw_v, rb_v, wgu_hbm, bgu_v, wd_hbm, bd_v, out_hbm, wg, wd, z_v, h_v, wbuf, g_v, gsend, acc, rs_v, x_v, ostage, bias_v, rwp_v, wg_s, wg_r, wd_s, wd_r, bias_s, bias_r, hg_s, hg_r, rs_s, rs_r, ld_sem, ld2_sem, in_sem, out_sem):
    tok, d_model = x_hbm.shape
    d_ff = wd_hbm.shape[1]
    groups = 2 * d_ff // COLS
    half_g = groups // 2
    blocks = d_model // COLS
    tm = tok // 2
    top_k = ids_v.shape[1]
    me = lax.axis_index('ep')
    core = lax.rem(me, 2)
    col = lax.rem(me // 2, RING)
    row = me // (2 * RING)
    away = 1 - 2 * core

    def dev(dy, dx, flip=0):
        other = 1 - core if flip else core
        return {'ep': (lax.rem(row + dy + RING, RING) * RING + lax.rem(col + dx + RING, RING)) * 2 + other}

    peers = [(2 * s, dc, f) for s, dc in ORDER for f in (0, 1)][1:]
    for dy, dx, f in peers + [(1, 0, 0), (-1, 0, 0)]:
        pl.semaphore_signal(pltpu.get_barrier_semaphore(), 1, device_id=dev(dy, dx, f), device_id_type=MESH)

    def remote(src, dst, ssem, rsem, where):
        return pltpu.make_async_remote_copy(src_ref=src, dst_ref=dst, send_sem=ssem, recv_sem=rsem, device_id=where, device_id_type=MESH)

    routes = {2: (0, 1), 4: (0, -1), 6: (0, 'y'), 10: (6, 1), 12: (6, -1)}
    relays = {8: ((2, 1), (4, -1)), 14: ((10, 1), (12, -1))}

    def route(q, part):
        if not isinstance(q, int):
            return q - 1, 'sib'
        if q % 2:
            return q - 1, 'sib'
        return relays[q][part] if q in relays else routes[q]

    def target(way):
        if way == 'sib':
            return dev(0, 0, 1)
        return dev(2, 0) if way == 'y' else dev(0, way)

    def gate_up(q, ch):
        src, way = route(q, ch)
        part = pl.ds(half_g * ch, half_g)
        own = isinstance(src, int) and src == 0
        return remote(wbuf.at[part] if own else wg.at[src, part], wg.at[q, part], wg_s.at[q, ch], wg_r.at[q, ch], target(way))

    def down(q, j, half=None):
        src, way = route(q, half)
        here = wd_hbm.at[0, :, pl.ds(pl.multiple_of(j * COLS, COLS), COLS)] if isinstance(src, int) and src == 0 else wd.at[src, j]
        there = wd.at[q, j]
        if half is not None:
            rows = pl.ds(d_ff // 2 * half, d_ff // 2)
            here, there = wd.at[src, j, rows], wd.at[q, j, rows]
        at = 0 if half is None else half
        return remote(here, there, wd_s.at[q, j, at], wd_r.at[q, j, at], target(way))

    def hidden_send():
        return remote(h_v.at[pl.ds(tok, tok)], h_v.at[pl.ds(0, tok)], hg_s.at[0], hg_r.at[0], dev(away, 0))

    def gates_send():
        return remote(gsend, g_v.at[pl.ds(0, tok)], hg_s.at[1], hg_r.at[1], dev(away, 0))

    def bias_send(q, where):
        return remote(bias_v.at[0], bias_v.at[q], bias_s.at[q], bias_r.at[q], where)

    def sum_send(j, t):
        return remote(acc.at[lax.rem(j, 2), t], rs_v.at[j, t], rs_s.at[j, t], rs_r.at[j, t], dev(-away, 0))

    raw = h_v.at[pl.ds(tok, tok)]
    load_w = pltpu.make_async_copy(wgu_hbm.at[0], raw.at[pl.ds(0, d_model)], in_sem.at[0])
    load_x = pltpu.make_async_copy(x_hbm, x_v, in_sem.at[1])
    load_w.start()
    load_x.start()

    ri = lax.broadcasted_iota(jnp.int32, (COLS, COLS), 0)
    ci = lax.broadcasted_iota(jnp.int32, (COLS, COLS), 1)
    split = jnp.where(ri == jnp.where(ci < COLS // 2, 2 * ci, 2 * ci - (COLS - 1)), 1.0, 0.0).astype(BF16)
    load_w.wait()
    for ch in range(2):
        for g in range(half_g * ch, half_g * (ch + 1)):
            wbuf[g] = jnp.dot(raw[pl.ds(0, d_model), COLS * g:COLS * (g + 1)], split, preferred_element_type=F32).astype(BF16)
        if ch == 0:
            pl.semaphore_wait(pltpu.get_barrier_semaphore(), len(peers) + 2)
        for q in (2, 4, 6, 1):
            gate_up(q, ch).start()

    for g in range(groups):
        b = jnp.dot(jnp.broadcast_to(bgu_v[:, COLS * g:COLS * (g + 1)], (16, COLS)), split, preferred_element_type=F32)
        bias_v[0, 2 * g:2 * g + 1, :] = b[0:1, :128]
        bias_v[0, 2 * g + 1:2 * g + 2, :] = b[0:1, 128:]
    for i in range(d_model // 128):
        bias_v[0, 2 * groups + i:2 * groups + i + 1, :] = bd_v[:, 128 * i:128 * (i + 1)].astype(F32)
    bias_msgs = []
    for s, dc in ORDER:
        for f in (0, 1):
            q = 2 * ORDER.index((s, (RING - dc) % RING)) + f
            if q:
                bias_msgs.append(bias_send(q, dev(2 * s, dc, f)))
                bias_msgs[-1].start()

    lane = lax.broadcasted_iota(jnp.int32, (1, 128), 1)
    slot = lane & (SLOTS - 1)
    class_row = jnp.where(lane < SLOTS, row, row + away + RING)
    far = jnp.zeros_like(lane)
    side = jnp.zeros_like(lane)
    for m, (s, dc) in enumerate(ORDER):
        far = jnp.where(slot // 2 == m, 2 * s, far)
        side = jnp.where(slot // 2 == m, dc, side)
    expert = (((class_row + far) & (RING - 1)) * RING + ((col + side) & (RING - 1))) * 2 + jnp.where((slot & 1) == 1, 1 - core, core)
    expert = jnp.where(lane < 2 * SLOTS, expert, -1)
    n_exp = rw_v.shape[1]
    pick = jnp.where(lax.broadcasted_iota(jnp.int32, (n_exp, 128), 0) == expert, 1.0, 0.0).astype(BF16)
    rwp_v[...] = jnp.dot(rw_v[...], pick, preferred_element_type=F32).astype(BF16)
    rb_p = jnp.dot(jnp.broadcast_to(rb_v[...], (16, n_exp)), pick, preferred_element_type=F32)[0:1]
    load_x.wait()
    norm = norm_v[...].astype(F32)
    tn = tok // 4

    @pl.loop(0, 4)
    def _(i):
        rows = pl.ds(pl.multiple_of(i * tn, tn), tn)
        own = pl.ds(pl.multiple_of(tok + i * tn, tn), tn)
        xf = x_v[rows, :].astype(F32)
        inv = lax.rsqrt(jnp.mean(xf * xf, axis=-1, keepdims=True) + EPSILON)
        hidden = (xf * inv * norm).astype(BF16)
        h_v[own, :] = hidden
        logits = jnp.dot(hidden, rwp_v[...], preferred_element_type=F32) + rb_p
        ids = ids_v[rows, :]
        chosen = ids[:, 0:1] == expert
        for e in range(1, top_k):
            chosen = chosen | (ids[:, e:e + 1] == expert)
        top = jnp.max(jnp.where(chosen, logits, -jnp.inf), axis=-1, keepdims=True)
        weight = jnp.where(chosen, jnp.exp(logits - top), 0.0)
        gates = weight / jnp.sum(weight, axis=-1, keepdims=True)
        g_v[own, :] = gates
        gsend[rows, :] = pltpu.roll(gates, 128 - SLOTS, 1)

    hidden_send().start()
    gates_send().start()
    for j in range(blocks):
        down(6, j).start()
        down(1, j).start()

    def q_of(s):
        return jnp.where(s < SLOTS, lax.rem(s, SLOTS // 2), SLOTS // 2 + (s - SLOTS) // 2)

    def own_of(s):
        return jnp.where(s < SLOTS, s < SLOTS // 2, lax.rem(s, 2) == 0)

    def set_of(s):
        return jnp.where(q_of(s) == 0, 0, 1 + lax.rem(s, 3))

    def weights_load(s):
        return pltpu.make_async_copy(wg.at[q_of(s)], wbuf.at[pl.ds(groups * set_of(s), groups)], ld_sem.at[set_of(s)])

    def landed(*msgs):
        for q, ch in msgs:
            gate_up(q, ch).wait_recv()

    def go(*msgs):
        for q, ch in msgs:
            gate_up(q, ch).start()

    def down_go(j, *qs):
        for q in qs:
            down(q, j).start()

    def down_landed(j, *qs):
        for q in qs:
            down(q, j).wait_recv()

    def event_1():
        landed((2, 0), (4, 0))
        go((8, 0), (3, 0), (5, 0))
        landed((2, 1), (4, 1))
        go((8, 1), (3, 1), (5, 1))

    def event_5():
        landed((6, 0), (6, 1))
        go((10, 0), (12, 0), (10, 1), (12, 1), (7, 0), (7, 1))

    def event_7():
        hidden_send().wait_recv()
        gates_send().wait_recv()

    def event_9():
        landed((8, 0), (8, 1))
        go((9, 0), (9, 1))

    def event_17():
        landed((10, 0), (12, 0))
        go((14, 0), (11, 0), (13, 0))

    def event_19():
        landed((10, 1), (12, 1))
        go((14, 1), (11, 1), (13, 1))
        for j in range(blocks):
            down_landed(j, 6)
            down_go(j, 7)
        down_go(0, 2, 4, 10, 12)
        down_go(1, 2, 4)

    def event_27():
        landed((14, 0), (14, 1))
        go((15, 0), (15, 1))

    events = {1: event_1, 5: event_5, 7: event_7, 9: event_9, 17: event_17, 19: event_19, 27: event_27}
    for msg in bias_msgs:
        msg.wait_recv()

    @pl.loop(0, 4 * SLOTS)
    def _(i):
        s = i // 2
        t = lax.rem(i, 2)
        q = q_of(s)

        @pl.when((t == 0) & (q > 0))
        def _():
            weights_load(s).wait()

        @pl.when(t == 1)
        def _():
            for at, event in events.items():
                pl.when(s == at)(event)
            nxt = s + 1
            q1 = q_of(nxt)

            @pl.when((lax.rem(q1, 2) == 1) & own_of(nxt) & (nxt < 2 * SLOTS))
            def _():
                for ch in range(2):
                    gate_up(q1, ch).wait_recv()

            @pl.when((q1 > 0) & (nxt < 2 * SLOTS))
            def _():
                weights_load(nxt).start()

        base = jnp.where(own_of(s), tok, 0)
        rows = pl.ds(pl.multiple_of(base + t * tm, tm), tm)
        w_at = groups * set_of(s)
        for g in range(groups):
            u = jnp.dot(h_v[rows, :], wbuf[w_at + g], preferred_element_type=F32)
            a = (u[:, :128] + bias_v[q, 2 * g:2 * g + 1, :]).astype(BF16)
            l = (u[:, 128:] + bias_v[q, 2 * g + 1:2 * g + 2, :]).astype(BF16)
            a = jnp.minimum(a, LIMIT).astype(F32)
            l = jnp.clip(l, -LIMIT, LIMIT).astype(F32)
            z_v[q, rows, 128 * g:128 * (g + 1)] = (a * jax.nn.sigmoid(ALPHA * a) * (l + 1.0)).astype(BF16)

    for q in (2, 4, 6, 1):
        for ch in range(2):
            gate_up(q, ch).wait_send()

    def down_load(j, q):
        spot = wbuf.at[SLOTS // 2 * lax.rem(j, 2) + q // 2, pl.ds(d_ff * (q % 2), d_ff)]
        src = wd_hbm.at[0, :, pl.ds(pl.multiple_of(j * COLS, COLS), COLS)] if q == 0 else wd.at[q, j]
        return pltpu.make_async_copy(src, spot, ld2_sem.at[lax.rem(j, 2), q])

    def direct(j):
        down_landed(j, 2, 4, 10, 12)
        for q in (8, 14):
            for half in range(2):
                down(q, j, half).start()

        @pl.when(j + 1 < blocks)
        def _():
            down_go(j + 1, 10, 12)

        @pl.when(j + 2 < blocks)
        def _():
            down_go(j + 2, 2, 4)

        down_go(j, 3, 5, 11, 13)
        for q in (0, 2, 4, 6, 10, 12):
            down_load(j, q).start()

    def relayed(j):
        for q in (8, 14):
            for half in range(2):
                down(q, j, half).wait_recv()
        down_go(j, 9, 15)
        for q in (8, 14):
            down_load(j, q).start()
        for q in (1, 3, 5, 7, 11, 13, 9, 15):
            down(q, j).wait_recv()
            down_load(j, q).start()
        for q in range(SLOTS):
            down_load(j, q).wait()

    def out_copy(j, t):
        cols = pl.ds(pl.multiple_of(j * COLS, COLS), COLS)
        return pltpu.make_async_copy(ostage.at[t], out_hbm.at[pl.ds(t * tm, tm), cols], out_sem.at[t])

    def finish(j, wait_out):
        cols = pl.ds(pl.multiple_of(j * COLS, COLS), COLS)
        for t in range(2):
            sum_send(j, t).wait_recv()
            if wait_out is not None:
                pl.when(wait_out)(lambda t=t: out_copy(j - 1, t).wait())
            total = acc[lax.rem(j, 2), 2 + t] + rs_v[j, t]
            ostage[t] = (x_v[pl.ds(t * tm, tm), cols].astype(F32) + total).astype(BF16)
            out_copy(j, t).start()

    direct(0)

    @pl.loop(0, blocks)
    def _(j):
        relayed(j)
        par = lax.rem(j, 2)

        @pl.loop(0, 4)
        def _(t):
            @pl.when((t < 2) & (j >= 2))
            def _():
                sum_send(j - 2, t).wait_send()

            @pl.when((t == 2) & (j + 1 < blocks))
            def _():
                direct(j + 1)

            @pl.when((t == 3) & (j >= 1))
            def _():
                finish(j - 1, j >= 2)

            rows = pl.ds(pl.multiple_of(t * tm, tm), tm)
            total = None
            for e in range(SLOTS):
                w = wbuf[SLOTS // 2 * par + e // 2, d_ff * (e % 2):d_ff * (e % 2 + 1), :]
                y = jnp.dot(z_v[e, rows, :], w, preferred_element_type=F32)
                b = jnp.concatenate([bias_v[e, pl.ds(2 * groups + 2 * j, 1), :], bias_v[e, pl.ds(2 * groups + 2 * j + 1, 1), :]], axis=1)
                y = (y + b).astype(BF16).astype(F32)
                p = g_v[rows, e:e + 1]
                term = jnp.where(p > 0, y * p, 0.0)
                total = term if total is None else total + term
            acc[par, t] = total

            @pl.when(t < 2)
            def _():
                sum_send(j, t).start()

    finish(blocks - 1, blocks >= 2)
    for t in range(2):
        out_copy(blocks - 1, t).wait()
        for j in range(max(blocks - 2, 0), blocks):
            sum_send(j, t).wait_send()

    for q in range(SLOTS):
        for ch in range(2):
            if q not in (0, 1, 2, 4, 6):
                gate_up(q, ch).wait_send()
        for j in range(blocks):
            if q in relays:
                for half in range(2):
                    down(q, j, half).wait_send()
            elif q:
                down(q, j).wait_send()
    for msg in bias_msgs:
        msg.wait_send()
    hidden_send().wait_send()
    gates_send().wait_send()


def solution(mesh):
    rows_spec = P(('dp', 'ep'), None)
    assert mesh.shape['ep'] == 2 * RING * RING

    def local_block(x_in, expert_ids, norm_weight, router_w, router_b, w_gate_up, b_gate_up, w_down, b_down):
        tok, d_model = x_in.shape
        d_ff = w_down.shape[1]
        assert w_gate_up.shape[0] == 1 and tok >= d_model
        groups, blocks, tm = 2 * d_ff // COLS, d_model // COLS, tok // 2
        hbm = pl.BlockSpec(memory_space=pltpu.HBM)
        vmem = pl.BlockSpec(memory_space=pltpu.VMEM)
        dma = pltpu.SemaphoreType.DMA
        wide = max(groups * 4, SLOTS * d_ff // d_model * 2)
        out = pl.pallas_call(
            kernel,
            out_shape=(
                jax.ShapeDtypeStruct((tok, d_model), BF16),
                jax.ShapeDtypeStruct((SLOTS, groups, d_model, COLS), BF16),
                jax.ShapeDtypeStruct((SLOTS, blocks, d_ff, COLS), BF16),
            ),
            in_specs=[hbm, vmem, vmem, vmem, vmem, hbm, vmem, hbm, vmem],
            out_specs=(hbm, hbm, hbm),
            scratch_shapes=[
                pltpu.VMEM((SLOTS, 2 * tok, d_ff), BF16),
                pltpu.VMEM((2 * tok, d_model), BF16),
                pltpu.VMEM((wide, d_model, COLS), BF16),
                pltpu.VMEM((2 * tok, 128), F32),
                pltpu.VMEM((tok, 128), F32),
                pltpu.VMEM((2, 4, tm, COLS), F32),
                pltpu.VMEM((blocks, 2, tm, COLS), F32),
                pltpu.VMEM((tok, d_model), BF16),
                pltpu.VMEM((2, tm, COLS), BF16),
                pltpu.VMEM((SLOTS, 2 * groups + d_model // 128, 128), F32),
                pltpu.VMEM((d_model, 128), BF16),
                dma((SLOTS, 2)),
                dma((SLOTS, 2)),
                dma((SLOTS, blocks, 2)),
                dma((SLOTS, blocks, 2)),
                dma((SLOTS,)),
                dma((SLOTS,)),
                dma((2,)),
                dma((2,)),
                dma((blocks, 2)),
                dma((blocks, 2)),
                dma((4,)),
                dma((2, SLOTS)),
                dma((2,)),
                dma((2,)),
            ],
            compiler_params=pltpu.CompilerParams(collective_id=0, has_side_effects=True, vmem_limit_bytes=67043328),
        )(x_in, expert_ids, norm_weight[None], router_w, router_b[None], w_gate_up, b_gate_up, w_down, b_down)
        return out[0]

    return jax.shard_map(local_block, mesh=mesh, in_specs=(rows_spec, rows_spec, P(), P(), P(), P('ep', None, None), P('ep', None), P('ep', None, None), P('ep', None)), out_specs=rows_spec, check_vma=False)
```

```python
import jax
import jax.numpy as jnp
from jax import lax
from jax.experimental import pallas as pl
from jax.experimental.pallas import tpu as pltpu
from jax.sharding import PartitionSpec as P

EPSILON = 1e-5
LIMIT = 7.0
ALPHA = 1.702
F32, BF16 = jnp.float32, jnp.bfloat16
MESH = pl.DeviceIdType.MESH
COLS = 256
RING = 4
ORDER = [(0, 0), (0, 3), (0, 1), (1, 0), (0, 2), (1, 3), (1, 1), (1, 2)]
SLOTS = 2 * len(ORDER)


def kernel(x_hbm, ids_v, norm_v, rw_v, rb_v, wgu_hbm, bgu_v, wd_hbm, bd_v, out_hbm, wg, wd, z_v, h_v, wbuf, g_v, gfar, gsend, acc, rs_v, x_v, ostage, bias_v, rwp_v, wg_s, wg_r, wd_s, wd_r, bias_s, bias_r, hg_s, hg_r, rs_s, rs_r, ld_sem, ld2_sem, in_sem, out_sem):
    tok, d_model = x_hbm.shape
    d_ff = wd_hbm.shape[1]
    groups = 2 * d_ff // COLS
    half_g = groups // 2
    blocks = d_model // COLS
    tm = tok // 2
    top_k = ids_v.shape[0]
    me = lax.axis_index('ep')
    core = lax.rem(me, 2)
    col = lax.rem(me // 2, RING)
    row = me // (2 * RING)
    away = 1 - 2 * core
    scope = jax.named_scope

    def dev(dy, dx, flip=0):
        other = 1 - core if flip else core
        return {'ep': (lax.rem(row + dy + RING, RING) * RING + lax.rem(col + dx + RING, RING)) * 2 + other}

    peers = [(2 * s, dc, f) for s, dc in ORDER for f in (0, 1)][1:]
    for dy, dx, f in peers + [(1, 0, 0), (-1, 0, 0)]:
        pl.semaphore_signal(pltpu.get_barrier_semaphore(), 1, device_id=dev(dy, dx, f), device_id_type=MESH)

    def remote(src, dst, ssem, rsem, where):
        return pltpu.make_async_remote_copy(src_ref=src, dst_ref=dst, send_sem=ssem, recv_sem=rsem, device_id=where, device_id_type=MESH)

    gate_up_way = {(2, 0): (0, 1), (2, 1): (0, 1), (4, 0): (0, -1), (4, 1): (0, -1), (6, 0): (0, 'y'), (6, 1): (0, 'y'), (8, 0): (4, -1), (8, 1): (2, 1),
                   (10, 0): (6, 1), (10, 1): (2, 'y'), (12, 0): (6, -1), (12, 1): (4, 'y'), (14, 0): (12, -1), (14, 1): (10, 1)}
    down_way = {2: (0, 1), 4: (0, -1), 6: (0, 'y'), (8, 0): (2, 1), (8, 1): (4, -1), 10: (6, 1), 12: (6, -1), (14, 0): (10, 1), (14, 1): (12, -1)}
    relayed_slots = (8, 14)

    def target(way):
        if way == 'sib':
            return dev(0, 0, 1)
        return dev(2, 0) if way == 'y' else dev(0, way)

    def gate_up(q, ch):
        src, way = gate_up_way.get((q, ch), (None, 'sib')) if isinstance(q, int) else (None, 'sib')
        part = pl.ds(half_g * ch, half_g)
        if src == 0 or (isinstance(q, int) and q == 1):
            here = wbuf.at[part]
        else:
            here = wg.at[q - 1 if src is None else src, part]
        return remote(here, wg.at[q, part], wg_s.at[q, ch], wg_r.at[q, ch], target(way))

    def down(q, j, half=None):
        src, way = down_way.get(q if half is None else (q, half), (q - 1, 'sib'))
        rows = slice(None) if half is None else pl.ds(d_ff // 2 * half, d_ff // 2)
        here = wd_hbm.at[0, :, pl.ds(pl.multiple_of(j * COLS, COLS), COLS)] if src == 0 else wd.at[src, j, rows]
        at = 0 if half is None else half
        return remote(here, wd.at[q, j, rows], wd_s.at[q, j, at], wd_r.at[q, j, at], target(way))

    def hidden_send():
        return remote(h_v.at[pl.ds(tok, tok)], h_v.at[pl.ds(0, tok)], hg_s.at[0], hg_r.at[0], dev(away, 0))

    def gates_send():
        return remote(gsend, gfar, hg_s.at[1], hg_r.at[1], dev(away, 0))

    def bias_send(q, where):
        return remote(bias_v.at[0], bias_v.at[q], bias_s.at[q], bias_r.at[q], where)

    def sum_send(j, t):
        return remote(acc.at[lax.rem(j, 2), t], rs_v.at[j, t], rs_s.at[j, t], rs_r.at[j, t], dev(-away, 0))

    raw = h_v.at[pl.ds(tok, tok)]
    load_w = pltpu.make_async_copy(wgu_hbm.at[0], raw.at[pl.ds(0, d_model)], in_sem.at[0])
    load_x = pltpu.make_async_copy(x_hbm, x_v, in_sem.at[1])
    load_w.start()
    load_x.start()

    ri = lax.broadcasted_iota(jnp.int32, (COLS, COLS), 0)
    ci = lax.broadcasted_iota(jnp.int32, (COLS, COLS), 1)
    split = jnp.where(ri == jnp.where(ci < COLS // 2, 2 * ci, 2 * ci - (COLS - 1)), 1.0, 0.0).astype(BF16)
    for g in range(groups):
        b = jnp.dot(jnp.broadcast_to(bgu_v[:, COLS * g:COLS * (g + 1)], (16, COLS)), split, preferred_element_type=F32)
        bias_v[0, 2 * g:2 * g + 1, :] = b[0:1, :128]
        bias_v[0, 2 * g + 1:2 * g + 2, :] = b[0:1, 128:]
    for i in range(d_model // 128):
        bias_v[0, 2 * groups + i:2 * groups + i + 1, :] = bd_v[:, 128 * i:128 * (i + 1)].astype(F32)
    with scope('load_w'):
        load_w.wait()
    for g in range(groups):
        wbuf[g] = jnp.dot(raw[pl.ds(0, d_model), COLS * g:COLS * (g + 1)], split, preferred_element_type=F32).astype(BF16)
    with scope('barrier'):
        pl.semaphore_wait(pltpu.get_barrier_semaphore(), len(peers) + 2)
    bias_msgs = []
    for s, dc in ORDER:
        for f in (0, 1):
            q = 2 * ORDER.index((s, (RING - dc) % RING)) + f
            if q:
                bias_msgs.append(bias_send(q, dev(2 * s, dc, f)))
                bias_msgs[-1].start()
    for q, ch in ((2, 1), (4, 0), (2, 0), (4, 1), (1, 0), (1, 1)):
        gate_up(q, ch).start()

    def expert_of(shape, dim):
        lane = lax.broadcasted_iota(jnp.int32, shape, dim)
        slot = lane & (SLOTS - 1)
        class_row = jnp.where(lane < SLOTS, row, row + away + RING)
        far = jnp.zeros_like(lane)
        side = jnp.zeros_like(lane)
        for m, (s, dc) in enumerate(ORDER):
            far = jnp.where(slot // 2 == m, 2 * s, far)
            side = jnp.where(slot // 2 == m, dc, side)
        expert = (((class_row + far) & (RING - 1)) * RING + ((col + side) & (RING - 1))) * 2 + jnp.where((slot & 1) == 1, 1 - core, core)
        return jnp.where(lane < 2 * SLOTS, expert, -1)

    n_exp = rw_v.shape[0]
    transposed = (((1,), (1,)), ((), ()))
    pick = jnp.where(expert_of((128, n_exp), 0) == lax.broadcasted_iota(jnp.int32, (128, n_exp), 1), 1.0, 0.0).astype(BF16)
    rwp_v[...] = jnp.dot(pick, rw_v[...], preferred_element_type=F32).astype(BF16)
    rb_p = lax.dot_general(jnp.broadcast_to(rb_v[...], (16, n_exp)), pick, transposed, preferred_element_type=F32)[0:1]
    expert = expert_of((1, 128), 1).astype(F32)
    load_x.wait()
    norm = norm_v[...].astype(F32)
    tn = tok // 4

    for i in range(4):
        rows = pl.ds(i * tn, tn)
        own = pl.ds(tok + i * tn, tn)
        xf = x_v[rows, :].astype(F32)
        inv = lax.rsqrt(jnp.mean(xf * xf, axis=-1, keepdims=True) + EPSILON)
        hidden = (xf * inv * norm).astype(BF16)
        h_v[own, :] = hidden
    hidden_send().start()
    for i in range(4):
        rows = pl.ds(i * tn, tn)
        own = pl.ds(tok + i * tn, tn)
        logits = lax.dot_general(h_v[own, :], rwp_v[...], transposed, preferred_element_type=F32) + rb_p
        ids = ids_v[:, i * tn:(i + 1) * tn].astype(F32).T
        chosen = ids[:, 0:1] == expert
        for e in range(1, top_k):
            chosen = chosen | (ids[:, e:e + 1] == expert)
        top = jnp.max(jnp.where(chosen, logits, -jnp.inf), axis=-1, keepdims=True)
        weight = jnp.where(chosen, jnp.exp(logits - top), 0.0)
        gates = weight / jnp.sum(weight, axis=-1, keepdims=True)
        g_v[own, :] = gates
        gsend[:, i * tn:(i + 1) * tn] = gates.T[SLOTS:2 * SLOTS]
    gates_send().start()
    for j in range(blocks):
        down(1, j).start()

    spans = [(0, lambda s: s // 2, lambda s: s % 2), (4, lambda s: s // 2, lambda s: s % 2),
             (8, lambda s: 2 + s, lambda s: 1 - s // 2), (12, lambda s: 2 + s, lambda s: s // 2),
             (16, lambda s: 6 + s, lambda s: 0), (18, lambda s: 8 + s // 2, lambda s: s % 2),
             (22, lambda s: 10 + s, lambda s: 1), (24, lambda s: 10 + s, lambda s: 0), (28, lambda s: 12 + s, lambda s: 1),
             (30, lambda s: 14 + s, lambda s: 1), (32, lambda s: 14 + s, lambda s: 0), (34, lambda s: 6 + s, lambda s: 1)]
    steps = 36

    def step_of(s):
        q, ch = 0, 0
        for at, q_at, ch_at in spans:
            r = jnp.maximum(s - at, 0)
            q = jnp.where(s >= at, q_at(r), q)
            ch = jnp.where(s >= at, ch_at(r), ch)
        return q, ch

    def buffer_of(s, q, ch):
        return jnp.where(q == 0, ch, 2 + lax.rem(s, 6))

    def weights_load(s):
        q, ch = step_of(s)
        b = buffer_of(s, q, ch)
        return pltpu.make_async_copy(wg.at[q, pl.ds(half_g * ch, half_g)], wbuf.at[pl.ds(half_g * b, half_g)], ld_sem.at[b])

    def landed(*msgs):
        for q, ch in msgs:
            gate_up(q, ch).wait_recv()

    def go(*msgs):
        for q, ch in msgs:
            gate_up(q, ch).start()

    def down_go(j, *qs):
        for q in qs:
            down(q, j).start()

    def down_landed(j, *qs):
        for q in qs:
            down(q, j).wait_recv()

    def down_relay_a(j):
        down_landed(j, 2, 4)
        for half in range(2):
            down(8, j, half).start()
        down_go(j, 3, 5)

    def down_relay_b(j):
        down_landed(j, 10, 12)
        for half in range(2):
            down(14, j, half).start()
        down_go(j, 11, 13)

    def event_3():
        hidden_send().wait_send()
        go((6, 0))
        hidden_send().wait_recv()

    def event_7():
        landed((2, 1), (4, 0))
        go((8, 1), (8, 0), (10, 1), (3, 1), (5, 0))

    def event_11():
        landed((2, 0), (4, 1))
        go((12, 1), (3, 0), (5, 1))

    def event_13():
        landed((6, 0))
        go((10, 0), (12, 0), (7, 0))
        down_go(0, 6)
        down_go(1, 6)
        go((6, 1))

    def event_17():
        down_go(0, 4)
        landed((8, 0), (8, 1))
        go((9, 0), (9, 1))
        down_go(2, 6)
        down_go(3, 6)

    def event_21():
        landed((10, 1))
        go((14, 1), (11, 1))
        down_go(0, 2)

    def event_23():
        landed((10, 0), (12, 0))
        go((14, 0), (11, 0), (13, 0))

    def event_27():
        landed((12, 1))
        go((13, 1))
        down_landed(0, 6)
        down_go(0, 10, 12, 7)
        down_go(1, 2, 4)

    def event_29():
        landed((14, 1))
        go((15, 1))

    def event_31():
        landed((14, 0))
        go((15, 0))
        down_relay_a(0)

    def event_33():
        landed((6, 1))
        go((7, 1))
        down_relay_b(0)
        for j in range(1, blocks):
            down_landed(j, 6)
            down_go(j, 7)
        down_go(1, 10, 12)
        down_go(2, 2, 4)

    events = {3: event_3, 7: event_7, 11: event_11, 13: event_13, 17: event_17, 21: event_21, 23: event_23, 27: event_27, 29: event_29, 31: event_31, 33: event_33}
    with scope('bias_wait'):
        for msg in bias_msgs:
            msg.wait_recv()

    @pl.loop(0, 8 + 2 * (steps - 8))
    def _(i):
        single = i < 8
        s = jnp.where(single, i, 4 + i // 2)
        q, ch = step_of(s)
        first = single | (lax.rem(i, 2) == 0)
        last = single | (lax.rem(i, 2) == 1)
        foreign = jnp.where(single, i // 4, lax.rem(i, 2))

        @pl.when(first & (q > 0))
        def _():
            with scope('load_wait'):
                weights_load(s).wait()

        @pl.when(last & (s < steps - 1))
        def _():
            @pl.when(lax.rem(s, 2) == 1)
            def _():
                for at, event in events.items():
                    @pl.when(s == at)
                    def _(event=event):
                        with scope(event.__name__):
                            event()

            q1, ch1 = step_of(s + 1)

            @pl.when((lax.rem(q1, 2) == 1) & ((s + 1 < 4) | (s + 1 >= 8)))
            def _():
                with scope('sib_wait'):
                    gate_up(q1, ch1).wait_recv()

            @pl.when(q1 > 0)
            def _():
                weights_load(s + 1).start()

        w_at = half_g * buffer_of(s, q, ch)
        bias_at = half_g * 2 * ch
        with scope('up'):
            for t in range(2):
                rows = pl.ds(pl.multiple_of((1 - foreign) * tok + t * tm, tm), tm)
                for g in range(half_g):
                    u = jnp.dot(h_v[rows, :], wbuf[w_at + g], preferred_element_type=F32)
                    a = (u[:, :128] + bias_v[q, pl.ds(bias_at + 2 * g, 1), :]).astype(BF16)
                    l = (u[:, 128:] + bias_v[q, pl.ds(bias_at + 2 * g + 1, 1), :]).astype(BF16)
                    a = jnp.minimum(a, LIMIT).astype(F32)
                    l = jnp.clip(l, -LIMIT, LIMIT).astype(F32)
                    z_v[q, rows, pl.ds(pl.multiple_of(128 * (half_g * ch + g), 128), 128)] = (a * jax.nn.sigmoid(ALPHA * a) * (l + 1.0)).astype(BF16)

    with scope('own_sent'):
        for q in (2, 4, 6, 1):
            for ch in range(2):
                gate_up(q, ch).wait_send()
    with scope('gates_in'):
        gates_send().wait_recv()
        for i in range(4):
            g_v[pl.ds(i * tn, tn), 0:SLOTS] = gfar[:, i * tn:(i + 1) * tn].T

    def down_load(j, q):
        spot = wbuf.at[SLOTS // 2 * lax.rem(j, 2) + q // 2, pl.ds(d_ff * (q % 2), d_ff)]
        src = wd_hbm.at[0, :, pl.ds(pl.multiple_of(j * COLS, COLS), COLS)] if q == 0 else wd.at[q, j]
        return pltpu.make_async_copy(src, spot, ld2_sem.at[lax.rem(j, 2), q])

    def relay(j):
        down_relay_a(j)
        down_relay_b(j)

        @pl.when(j + 1 < blocks)
        def _():
            down_go(j + 1, 10, 12)

        @pl.when(j + 2 < blocks)
        def _():
            down_go(j + 2, 2, 4)

    def load_early(j):
        for q in (0, 2, 4, 6, 10, 12):
            down_load(j, q).start()

    def load_sib(j):
        for q in (1, 3, 5, 7, 11, 13):
            down(q, j).wait_recv()
            down_load(j, q).start()

    def load_late(j):
        for q in relayed_slots:
            for half in range(2):
                down(q, j, half).wait_recv()
            down_go(j, q + 1)
            down_load(j, q).start()
        for q in relayed_slots:
            down(q + 1, j).wait_recv()
            down_load(j, q + 1).start()
        for q in range(SLOTS):
            down_load(j, q).wait()

    def out_copy(j, t):
        cols = pl.ds(pl.multiple_of(j * COLS, COLS), COLS)
        return pltpu.make_async_copy(ostage.at[t], out_hbm.at[pl.ds(t * tm, tm), cols], out_sem.at[t])

    def finish(j, wait_out):
        cols = pl.ds(pl.multiple_of(j * COLS, COLS), COLS)
        for t in range(2):
            sum_send(j, t).wait_recv()
            pl.when(wait_out)(lambda t=t: out_copy(j - 1, t).wait())
            total = acc[lax.rem(j, 2), 2 + t] + rs_v[j, t]
            ostage[t] = (x_v[pl.ds(t * tm, tm), cols].astype(F32) + total).astype(BF16)
            out_copy(j, t).start()

    load_early(0)
    load_sib(0)

    @pl.loop(0, blocks)
    def _(j):
        with scope('load_late'):
            load_late(j)
        par = lax.rem(j, 2)

        @pl.loop(0, 4)
        def _(t):
            @pl.when((t < 2) & (j >= 2))
            def _():
                sum_send(j - 2, t).wait_send()

            @pl.when((t == 1) & (j + 1 < blocks))
            def _():
                with scope('relay'):
                    relay(j + 1)
                    load_early(j + 1)

            @pl.when((t == 2) & (j + 1 < blocks))
            def _():
                with scope('load_sib'):
                    load_sib(j + 1)

            @pl.when((t == 3) & (j >= 1))
            def _():
                with scope('finish'):
                    finish(j - 1, j >= 2)

            rows = pl.ds(pl.multiple_of(t * tm, tm), tm)
            with scope('down'):
                total = None
                for e in range(SLOTS):
                    w = wbuf[SLOTS // 2 * par + e // 2, d_ff * (e % 2):d_ff * (e % 2 + 1), :]
                    y = jnp.dot(z_v[e, rows, :], w, preferred_element_type=F32)
                    b = jnp.concatenate([bias_v[e, pl.ds(2 * groups + 2 * j, 1), :], bias_v[e, pl.ds(2 * groups + 2 * j + 1, 1), :]], axis=1)
                    y = (y + b).astype(BF16).astype(F32)
                    p = g_v[rows, e:e + 1]
                    term = jnp.where(p > 0, y * p, 0.0)
                    total = term if total is None else total + term
                acc[par, t] = total

            @pl.when(t < 2)
            def _():
                sum_send(j, t).start()

    with scope('last_finish'):
        finish(blocks - 1, blocks >= 2)
        for t in range(2):
            out_copy(blocks - 1, t).wait()
    with scope('drain'):
        for t in range(2):
            for j in range(max(blocks - 2, 0), blocks):
                sum_send(j, t).wait_send()
        for q in range(SLOTS):
            for ch in range(2):
                if q not in (0, 1, 2, 4, 6):
                    gate_up(q, ch).wait_send()
            for j in range(blocks):
                if q in relayed_slots:
                    for half in range(2):
                        down(q, j, half).wait_send()
                elif q:
                    down(q, j).wait_send()
        for msg in bias_msgs:
            msg.wait_send()
        gates_send().wait_send()


def solution(mesh):
    rows_spec = P(('dp', 'ep'), None)
    assert mesh.shape['ep'] == 2 * RING * RING

    def local_block(x_in, expert_ids, norm_weight, router_w, router_b, w_gate_up, b_gate_up, w_down, b_down):
        tok, d_model = x_in.shape
        d_ff = w_down.shape[1]
        assert w_gate_up.shape[0] == 1 and tok >= d_model
        groups, blocks, tm = 2 * d_ff // COLS, d_model // COLS, tok // 2
        hbm = pl.BlockSpec(memory_space=pltpu.HBM)
        vmem = pl.BlockSpec(memory_space=pltpu.VMEM)
        dma = pltpu.SemaphoreType.DMA
        wide = max(groups * 4, SLOTS * d_ff // d_model * 2)
        out = pl.pallas_call(
            kernel,
            out_shape=(
                jax.ShapeDtypeStruct((tok, d_model), BF16),
                jax.ShapeDtypeStruct((SLOTS, groups, d_model, COLS), BF16),
                jax.ShapeDtypeStruct((SLOTS, blocks, d_ff, COLS), BF16),
            ),
            in_specs=[hbm, vmem, vmem, vmem, vmem, hbm, vmem, hbm, vmem],
            out_specs=(hbm, hbm, hbm),
            scratch_shapes=[
                pltpu.VMEM((SLOTS, 2 * tok, d_ff), BF16),
                pltpu.VMEM((2 * tok, d_model), BF16),
                pltpu.VMEM((wide, d_model, COLS), BF16),
                pltpu.VMEM((2 * tok, 128), F32),
                pltpu.VMEM((SLOTS, tok), F32),
                pltpu.VMEM((SLOTS, tok), F32),
                pltpu.VMEM((2, 4, tm, COLS), F32),
                pltpu.VMEM((blocks, 2, tm, COLS), F32),
                pltpu.VMEM((tok, d_model), BF16),
                pltpu.VMEM((2, tm, COLS), BF16),
                pltpu.VMEM((SLOTS, 2 * groups + d_model // 128, 128), F32),
                pltpu.VMEM((128, d_model), BF16),
                dma((SLOTS, 2)),
                dma((SLOTS, 2)),
                dma((SLOTS, blocks, 2)),
                dma((SLOTS, blocks, 2)),
                dma((SLOTS,)),
                dma((SLOTS,)),
                dma((2,)),
                dma((2,)),
                dma((blocks, 2)),
                dma((blocks, 2)),
                dma((8,)),
                dma((2, SLOTS)),
                dma((2,)),
                dma((2,)),
            ],
            compiler_params=pltpu.CompilerParams(collective_id=0, has_side_effects=True, vmem_limit_bytes=67043328),
        )(x_in, expert_ids.T, norm_weight[None], router_w.T, router_b[None], w_gate_up, b_gate_up, w_down, b_down)
        return out[0]

    return jax.shard_map(local_block, mesh=mesh, in_specs=(rows_spec, rows_spec, P(), P(), P(), P('ep', None, None), P('ep', None), P('ep', None, None), P('ep', None)), out_specs=rows_spec, check_vma=False)
```

```python
import jax
import jax.numpy as jnp
from jax import lax
from jax.experimental import pallas as pl
from jax.experimental.pallas import tpu as pltpu
from jax.sharding import PartitionSpec as P

EPSILON = 1e-5
LIMIT = 7.0
ALPHA = 1.702
F32, BF16 = jnp.float32, jnp.bfloat16
MESH = pl.DeviceIdType.MESH
COLS = 256
RING = 4
ORDER = [(0, 0), (0, 3), (0, 1), (1, 0), (0, 2), (1, 3), (1, 1), (1, 2)]
SLOTS = 2 * len(ORDER)
NAMES = 'aAbBcCdDeEfFgGhH'
GATE_UP_WAYS = 'b0a+,b1a+,c0a-,c1a-,d0ay,d1ay,e0c-,e1b+,' + 'f0d+,f1by,g0d-,g1cy,h0g-,h1f+'
DOWN_WAYS = 'b.a+,c.a-,d.ay,e0b+,e1c-,f.d+,g.d-,h0f+,h1g-'
STEPS = 'a0a1A0A1a0a1A0A1b1B1c0C0b0B0c1C1d0D0' + 'e0e1E0E1f1F1f0F0g0G0g1G1h1H1h0H0d1D1'
PHASE_1 = {
    3: ['~,!d0,?~'],
    7: ['?b1,?c0,!e1,!e0,!f1,!B1,!C0'],
    11: ['?b0,?c1,!g1,!B0,!C1'],
    13: ['?d0,!f0,!g0,!D0,!d.0,!d1'],
    17: ['!c.0,?e0,?e1,!E0,!E1,!d.1,!d.2,!d.3'],
    21: ['?f1,!h1,!F1,!b.0'],
    23: ['?f0,?g0,!h0,!F0,!G0'],
    27: ['?g1,!G1,?d.0,!f.0,!g.0,!D.0,!b.1,!c.1'],
    29: ['?h1,!H1'],
    31: ['?h0,!H0', 'r0'],
    33: ['s0,?d1,!D1,?d.1,!f.1,!g.1,!b.2,!c.2,!D.1'],
}
PHASE_2 = {
    0: ['i0,j0,k0,l0,w0'],
    1: ['r1,s1,?d.2,!f.2,!g.2,!b.3,!c.3,!D.2,i1'],
    2: ['j1'],
    4: ['k1,l1,w1'],
    5: ['r2,s2,?d.3,!f.3,!g.3,!D.3,i2'],
    6: ['j2'],
    7: ['r3'],
    8: ['k2,l2,w2'],
    9: ['s3,i3'],
    10: ['j3'],
    12: ['k3,l3,w3'],
}
SHORT = {'r': '?b,?c,!e,!B,!C', 's': '?f,?g,!h,!F,!G', 'i': '<a,<b,<c,<d,<f,<g', 'j': '?A,<A,?B,<B,?C,<C,?D,<D,?F,<F,?G,<G',
         'k': '?e,!E,<e,?h,!H,<h', 'l': '?E,<E,?H,<H'}


def kernel(*refs):
    slots, blocks = refs[10].shape[0], refs[11].shape[1]
    counts = [(slots, 2), (slots, 2), (slots, blocks, 2), (slots, blocks, 2), (slots,), (slots,), (2,), (2,), (blocks, 2), (blocks, 2), (8,), (2, slots), (2,), (2,)]
    pl.run_scoped(lambda *sems: body(*refs, *sems), *[pltpu.SemaphoreType.DMA(c) for c in counts])


def body(x_hbm, ids_v, norm_v, rw_v, rb_v, wgu_hbm, bgu_v, wd_hbm, bd_v, out_hbm, wg, wd, z_v, h_v, wbuf, g_v, gfar, gsend, acc, rs_v, x_v, ostage, bias_v, rwp_v, wg_s, wg_r, wd_s, wd_r, bias_s, bias_r, hg_s, hg_r, rs_s, rs_r, ld_sem, ld2_sem, in_sem, out_sem):
    tok, d_model = x_hbm.shape
    d_ff = wd_hbm.shape[1]
    groups = 2 * d_ff // COLS
    half_g = groups // 2
    blocks = d_model // COLS
    tm = tok // 2
    top_k = ids_v.shape[0]
    me = lax.axis_index('ep')
    core = lax.rem(me, 2)
    col = lax.rem(me // 2, RING)
    row = me // (2 * RING)
    away = 1 - 2 * core
    scope = jax.named_scope

    def dev(dy, dx, flip=0):
        other = 1 - core if flip else core
        return {'ep': (lax.rem(row + dy + RING, RING) * RING + lax.rem(col + dx + RING, RING)) * 2 + other}

    peers = [(2 * s, dc, f) for s, dc in ORDER for f in (0, 1)][1:]
    for dy, dx, f in peers + [(1, 0, 0), (-1, 0, 0)]:
        pl.semaphore_signal(pltpu.get_barrier_semaphore(), 1, device_id=dev(dy, dx, f), device_id_type=MESH)

    def remote(src, dst, ssem, rsem, where):
        return pltpu.make_async_remote_copy(src_ref=src, dst_ref=dst, send_sem=ssem, recv_sem=rsem, device_id=where, device_id_type=MESH)

    def ways(table):
        return {(NAMES.index(m[0]), m[1]): (NAMES.index(m[2]), m[3]) for m in table.split(',')}

    gate_up_way, down_way = ways(GATE_UP_WAYS), ways(DOWN_WAYS)
    relayed_slots = [NAMES.index(n) for n in 'eh']

    def target(way):
        if way == 's':
            return dev(0, 0, 1)
        return dev(2, 0) if way == 'y' else dev(0, 1 if way == '+' else -1)

    def gate_up(q, ch):
        static = isinstance(q, int)
        src, way = gate_up_way.get((q, str(ch)), (q - 1, 's')) if static else (q - 1, 's')
        part = pl.ds(half_g * ch, half_g)
        here = wbuf.at[part] if static and src == 0 else wg.at[src, part]
        return remote(here, wg.at[q, part], wg_s.at[q, ch], wg_r.at[q, ch], target(way))

    def down(q, j):
        def one(half):
            src, way = down_way.get((q, half), (q - 1, 's'))
            rows = slice(None) if half == '.' else pl.ds(d_ff // 2 * int(half), d_ff // 2)
            here = wd_hbm.at[0, :, pl.ds(j * COLS, COLS)] if src == 0 else wd.at[src, j, rows]
            at = 0 if half == '.' else int(half)
            return remote(here, wd.at[q, j, rows], wd_s.at[q, j, at], wd_r.at[q, j, at], target(way))

        return [one(half) for half in ('01' if q in relayed_slots else '.')]

    def hidden_send():
        return remote(h_v.at[pl.ds(tok, tok)], h_v.at[pl.ds(0, tok)], hg_s.at[0], hg_r.at[0], dev(away, 0))

    def gates_send():
        return remote(gsend, gfar, hg_s.at[1], hg_r.at[1], dev(away, 0))

    def bias_send(q, where):
        return remote(bias_v.at[0], bias_v.at[q], bias_s.at[q], bias_r.at[q], where)

    def sum_send(j, t):
        return remote(acc.at[lax.rem(j, 2), t], rs_v.at[j, t], rs_s.at[j, t], rs_r.at[j, t], dev(-away, 0))

    raw = h_v.at[pl.ds(tok, tok)]
    load_w = pltpu.make_async_copy(wgu_hbm.at[0], raw.at[pl.ds(0, d_model)], in_sem.at[0])
    load_x = pltpu.make_async_copy(x_hbm, x_v, in_sem.at[1])
    load_w.start()
    load_x.start()

    ri = lax.broadcasted_iota(jnp.int32, (COLS, COLS), 0)
    ci = lax.broadcasted_iota(jnp.int32, (COLS, COLS), 1)
    split = jnp.where(ri == jnp.where(ci < COLS // 2, 2 * ci, 2 * ci - (COLS - 1)), 1.0, 0.0).astype(BF16)
    for g in range(groups):
        b = jnp.dot(jnp.broadcast_to(bgu_v[:, COLS * g:COLS * (g + 1)], (16, COLS)), split, preferred_element_type=F32)
        bias_v[0, 2 * g:2 * g + 1, :] = b[0:1, :128]
        bias_v[0, 2 * g + 1:2 * g + 2, :] = b[0:1, 128:]
    for i in range(d_model // 128):
        bias_v[0, 2 * groups + i:2 * groups + i + 1, :] = bd_v[:, 128 * i:128 * (i + 1)].astype(F32)
    with scope('load_w'):
        load_w.wait()
    for g in range(groups):
        wbuf[g] = jnp.dot(raw[pl.ds(0, d_model), COLS * g:COLS * (g + 1)], split, preferred_element_type=F32).astype(BF16)
    with scope('barrier'):
        pl.semaphore_wait(pltpu.get_barrier_semaphore(), len(peers) + 2)
    bias_msgs = []
    for s, dc in ORDER:
        for f in (0, 1):
            q = 2 * ORDER.index((s, (RING - dc) % RING)) + f
            if q:
                bias_msgs.append(bias_send(q, dev(2 * s, dc, f)))
                bias_msgs[-1].start()
    for name in 'b1,c0,b0,c1,A0,A1'.split(','):
        gate_up(NAMES.index(name[0]), int(name[1])).start()

    def expert_of(shape, dim):
        lane = lax.broadcasted_iota(jnp.int32, shape, dim)
        slot = lane & (SLOTS - 1)
        class_row = jnp.where(lane < SLOTS, row, row + away + RING)
        far = jnp.zeros_like(lane)
        side = jnp.zeros_like(lane)
        for m, (s, dc) in enumerate(ORDER):
            far = jnp.where(slot // 2 == m, 2 * s, far)
            side = jnp.where(slot // 2 == m, dc, side)
        expert = (((class_row + far) & (RING - 1)) * RING + ((col + side) & (RING - 1))) * 2 + jnp.where((slot & 1) == 1, 1 - core, core)
        return jnp.where(lane < 2 * SLOTS, expert, -1)

    n_exp = rw_v.shape[0]
    transposed = (((1,), (1,)), ((), ()))
    pick = jnp.where(expert_of((128, n_exp), 0) == lax.broadcasted_iota(jnp.int32, (128, n_exp), 1), 1.0, 0.0).astype(BF16)
    rwp_v[...] = jnp.dot(pick, rw_v[...], preferred_element_type=F32).astype(BF16)
    rb_p = lax.dot_general(jnp.broadcast_to(rb_v[...], (16, n_exp)), pick, transposed, preferred_element_type=F32)[0:1]
    expert = expert_of((1, 128), 1).astype(F32)
    load_x.wait()
    norm = jnp.concatenate([norm_v[i:i + 1, :].astype(F32) for i in range(d_model // 128)], axis=1)
    tn = tok // 4

    for i in range(4):
        rows = pl.ds(i * tn, tn)
        own = pl.ds(tok + i * tn, tn)
        xf = x_v[rows, :].astype(F32)
        inv = lax.rsqrt(jnp.mean(xf * xf, axis=-1, keepdims=True) + EPSILON)
        hidden = (xf * inv * norm).astype(BF16)
        h_v[own, :] = hidden
    hidden_send().start()
    for i in range(4):
        rows = pl.ds(i * tn, tn)
        own = pl.ds(tok + i * tn, tn)
        logits = lax.dot_general(h_v[own, :], rwp_v[...], transposed, preferred_element_type=F32) + rb_p
        ids = ids_v[:, i * tn:(i + 1) * tn].astype(F32).T
        chosen = ids[:, 0:1] == expert
        for e in range(1, top_k):
            chosen = chosen | (ids[:, e:e + 1] == expert)
        top = jnp.max(jnp.where(chosen, logits, -jnp.inf), axis=-1, keepdims=True)
        weight = jnp.where(chosen, jnp.exp(logits - top), 0.0)
        gates = weight / jnp.sum(weight, axis=-1, keepdims=True)
        g_v[own, :] = gates
        gsend[:, i * tn:(i + 1) * tn] = gates.T[SLOTS:2 * SLOTS]
    gates_send().start()
    for j in range(blocks):
        for msg in down(1, j):
            msg.start()

    codes = [2 * NAMES.index(n) + int(ch) for n, ch in zip(STEPS[::2], STEPS[1::2])]
    steps = len(codes)
    per, bits = 6, 5
    words = [sum(c << bits * i for i, c in enumerate(codes[at:at + per])) for at in range(0, steps, per)]

    def step_of(s):
        word = jnp.int32(words[0])
        for i, w in enumerate(words[1:]):
            word = jnp.where(s >= per * (i + 1), w, word)
        code = lax.shift_right_logical(word, bits * lax.rem(s, per)) & ((1 << bits) - 1)
        return code // 2, lax.rem(code, 2)

    def buffer_of(s, q, ch):
        return jnp.where(q == 0, ch, 2 + lax.rem(s, 6))

    def weights_load(s):
        q, ch = step_of(s)
        b = buffer_of(s, q, ch)
        return pltpu.make_async_copy(wg.at[q, pl.ds(half_g * ch, half_g)], wbuf.at[pl.ds(half_g * b, half_g)], ld_sem.at[b])

    def down_load(j, q):
        spot = wbuf.at[SLOTS // 2 * (j % 2) + q // 2, pl.ds(d_ff * (q % 2), d_ff)]
        src = wd_hbm.at[0, :, pl.ds(j * COLS, COLS)] if q == 0 else wd.at[q, j]
        return pltpu.make_async_copy(src, spot, ld2_sem.at[j % 2, q])

    def act(text):
        for word in text.split(','):
            what, name, rest = word[0], word[1:2], word[2:]
            if what == '~':
                hidden_send().wait_send()
            elif name == '~':
                hidden_send().wait_recv()
            elif what == 'w':
                for q in range(SLOTS):
                    down_load(int(name), q).wait()
            elif what in SHORT:
                if int(name) < blocks:
                    act(','.join(w + '.' + name for w in SHORT[what].split(',')))
            elif rest[0] != '.':
                msg = gate_up(NAMES.index(name), int(rest))
                msg.start() if what == '!' else msg.wait_recv()
            elif int(rest[1:]) < blocks:
                q, j = NAMES.index(name), int(rest[1:])
                if what == '<':
                    down_load(j, q).start()
                else:
                    for msg in down(q, j):
                        msg.start() if what == '!' else msg.wait_recv()

    def events(table, now):
        for at, texts in table.items():
            @pl.when(now == at)
            def _(at=at, texts=texts):
                with scope('event_' + str(at)):
                    for text in texts:
                        act(text)

    with scope('bias_wait'):
        for msg in bias_msgs:
            msg.wait_recv()

    @pl.loop(0, 8 + 2 * (steps - 8))
    def _(i):
        single = i < 8
        s = jnp.where(single, i, 4 + i // 2)
        q, ch = step_of(s)
        first = single | (lax.rem(i, 2) == 0)
        last = single | (lax.rem(i, 2) == 1)
        foreign = jnp.where(single, i // 4, lax.rem(i, 2))

        @pl.when(first & (q > 0))
        def _():
            with scope('load_wait'):
                weights_load(s).wait()

        @pl.when(last & (s < steps - 1))
        def _():
            @pl.when(lax.rem(s, 2) == 1)
            def _():
                events(PHASE_1, s)

            q1, ch1 = step_of(s + 1)

            @pl.when((lax.rem(q1, 2) == 1) & ((s < 3) | (s >= 7)))
            def _():
                with scope('sib_wait'):
                    gate_up(q1, ch1).wait_recv()

            @pl.when(q1 > 0)
            def _():
                weights_load(s + 1).start()

        w_at = half_g * buffer_of(s, q, ch)
        bias_at = half_g * 2 * ch
        with scope('up'):
            for t in range(2):
                rows = pl.ds(pl.multiple_of((1 - foreign) * tok + t * tm, tm), tm)
                for g in range(half_g):
                    u = jnp.dot(h_v[rows, :], wbuf[w_at + g], preferred_element_type=F32)
                    a = (u[:, :128] + bias_v[q, pl.ds(bias_at + 2 * g, 1), :]).astype(BF16)
                    l = (u[:, 128:] + bias_v[q, pl.ds(bias_at + 2 * g + 1, 1), :]).astype(BF16)
                    a = jnp.minimum(a, LIMIT).astype(F32)
                    l = jnp.clip(l, -LIMIT, LIMIT).astype(F32)
                    z_v[q, rows, pl.ds(pl.multiple_of(128 * (half_g * ch + g), 128), 128)] = (a * jax.nn.sigmoid(ALPHA * a) * (l + 1.0)).astype(BF16)

    with scope('own_sent'):
        for q in (2, 4, 6, 1):
            for ch in range(2):
                gate_up(q, ch).wait_send()
    with scope('gates_in'):
        gates_send().wait_recv()
        for i in range(4):
            g_v[pl.ds(i * tn, tn), 0:SLOTS] = gfar[:, i * tn:(i + 1) * tn].T

    def out_copy(j, t):
        cols = pl.ds(pl.multiple_of(j * COLS, COLS), COLS)
        return pltpu.make_async_copy(ostage.at[t], out_hbm.at[pl.ds(t * tm, tm), cols], out_sem.at[t])

    def finish(j, wait_out):
        cols = pl.ds(pl.multiple_of(j * COLS, COLS), COLS)
        for t in range(2):
            sum_send(j, t).wait_recv()
            pl.when(wait_out)(lambda t=t: out_copy(j - 1, t).wait())
            total = acc[lax.rem(j, 2), 2 + t] + rs_v[j, t]
            ostage[t] = (x_v[pl.ds(t * tm, tm), cols].astype(F32) + total).astype(BF16)
            out_copy(j, t).start()

    @pl.loop(0, blocks)
    def _(j):
        par = lax.rem(j, 2)

        @pl.loop(0, 4)
        def _(t):
            @pl.when((t < 2) & (j >= 2))
            def _():
                sum_send(j - 2, t).wait_send()

            events({at: texts for at, texts in PHASE_2.items() if at < 4 * blocks}, 4 * j + t)

            @pl.when((t == 3) & (j >= 1))
            def _():
                with scope('finish'):
                    finish(j - 1, j >= 2)

            rows = pl.ds(pl.multiple_of(t * tm, tm), tm)
            with scope('down'):
                total = None
                for e in range(SLOTS):
                    w = wbuf[SLOTS // 2 * par + e // 2, d_ff * (e % 2):d_ff * (e % 2 + 1), :]
                    y = jnp.dot(z_v[e, rows, :], w, preferred_element_type=F32)
                    b = jnp.concatenate([bias_v[e, pl.ds(2 * groups + 2 * j, 1), :], bias_v[e, pl.ds(2 * groups + 2 * j + 1, 1), :]], axis=1)
                    y = (y + b).astype(BF16).astype(F32)
                    p = g_v[rows, e:e + 1]
                    term = jnp.where(p > 0, y * p, 0.0)
                    total = term if total is None else total + term
                acc[par, t] = total

            @pl.when(t < 2)
            def _():
                sum_send(j, t).start()

    with scope('last_finish'):
        finish(blocks - 1, blocks >= 2)
        for t in range(2):
            out_copy(blocks - 1, t).wait()
    with scope('drain'):
        for t in range(2):
            for j in range(max(blocks - 2, 0), blocks):
                sum_send(j, t).wait_send()
        for q in range(SLOTS):
            for ch in range(2):
                if q not in (0, 1, 2, 4, 6):
                    gate_up(q, ch).wait_send()
            for j in range(blocks if q else 0):
                for msg in down(q, j):
                    msg.wait_send()
        for msg in bias_msgs:
            msg.wait_send()
        gates_send().wait_send()


def solution(mesh):
    rows_spec = P(('dp', 'ep'), None)
    assert mesh.shape['ep'] == 2 * RING * RING

    def local_block(x_in, expert_ids, norm_weight, router_w, router_b, w_gate_up, b_gate_up, w_down, b_down):
        tok, d_model = x_in.shape
        d_ff = w_down.shape[1]
        assert w_gate_up.shape[0] == 1 and tok >= d_model
        groups, blocks, tm = 2 * d_ff // COLS, d_model // COLS, tok // 2
        hbm = pl.BlockSpec(memory_space=pltpu.HBM)
        vmem = pl.BlockSpec(memory_space=pltpu.VMEM)
        wide = max(groups * 4, SLOTS * d_ff // d_model * 2)
        out = pl.pallas_call(
            kernel,
            out_shape=(
                jax.ShapeDtypeStruct((tok, d_model), BF16),
                jax.ShapeDtypeStruct((SLOTS, groups, d_model, COLS), BF16),
                jax.ShapeDtypeStruct((SLOTS, blocks, d_ff, COLS), BF16),
            ),
            in_specs=[hbm, vmem, vmem, vmem, vmem, hbm, vmem, hbm, vmem],
            out_specs=(hbm, hbm, hbm),
            scratch_shapes=[
                pltpu.VMEM((SLOTS, 2 * tok, d_ff), BF16),
                pltpu.VMEM((2 * tok, d_model), BF16),
                pltpu.VMEM((wide, d_model, COLS), BF16),
                pltpu.VMEM((2 * tok, 128), F32),
                pltpu.VMEM((SLOTS, tok), F32),
                pltpu.VMEM((SLOTS, tok), F32),
                pltpu.VMEM((2, 4, tm, COLS), F32),
                pltpu.VMEM((blocks, 2, tm, COLS), F32),
                pltpu.VMEM((tok, d_model), BF16),
                pltpu.VMEM((2, tm, COLS), BF16),
                pltpu.VMEM((SLOTS, 2 * groups + d_model // 128, 128), F32),
                pltpu.VMEM((128, d_model), BF16),
            ],
            compiler_params=pltpu.CompilerParams(collective_id=0, has_side_effects=True, vmem_limit_bytes=67043328),
        )(x_in, expert_ids.T, norm_weight.reshape(-1, 128), router_w.T, router_b[None], w_gate_up, b_gate_up, w_down, b_down)
        return out[0]

    return jax.shard_map(local_block, mesh=mesh, in_specs=(rows_spec, rows_spec, P(), P(), P(), P('ep', None, None), P('ep', None), P('ep', None, None), P('ep', None)), out_specs=rows_spec, check_vma=False)
```

```python
import jax
import jax.numpy as jnp
from jax import lax
from jax.experimental import pallas as pl
from jax.experimental.pallas import tpu as pltpu
from jax.sharding import PartitionSpec as P

EPSILON = 1e-5
LIMIT = 7.0
ALPHA = 1.702
F32, BF16 = jnp.float32, jnp.bfloat16
MESH = pl.DeviceIdType.MESH
COLS = 256
RING = 4
ORDER = [(0, 0), (0, 3), (0, 1), (1, 0), (0, 2), (1, 3), (1, 1), (1, 2)]
SLOTS = 2 * len(ORDER)
SCRATCH = 18
NAMES = 'aAbBcCdDeEfFgGhH'
GATE_UP_WAYS = 'b0a+,b1a+,c0a-,c1a-,d0ay,d1ay,e0c-,e1b+,' + 'f0d+,f1by,g0d-,g1cy,h0g-,h1f+'
DOWN_WAYS = 'b.a+,c.a-,d.ay,e0b+,e1c-,f.d+,g.d-,h0f+,h1g-'
FIRST_WAYS = 'h0ey,h1ey'
STEPS = 'a0a1A0A1a0a1A0A1b1B1c0C0b0B0c1C1d0D0' + 'e0e1E0E1f1F1f0F0g0G0g1G1h1H1h0H0d1D1'
PHASE_1 = {
    3: ['~,!d0,?~'],
    7: ['?b1,?c0,!e1,!e0,!f1,!B1,!C0'],
    11: ['?b0,?c1,!g1,!B0,!C1'],
    13: ['?d0,!f0,!g0,!D0,!d.0,!d1'],
    17: ['!c.0,?e0,?e1,!E0,!E1,!d.1'],
    21: ['?f1,!h1,!F1,!b.0'],
    23: ['?f0,?g0,!h0,!F0,!G0'],
    27: ['?g1,!G1,?d.0,!f.0,!g.0,!D.0'],
    29: ['?h1,!H1'],
    31: ['?h0,!H0', 'r0,!b.1,!c.1'],
    33: ['?d1,!D1,?d.1,!f.1,!g.1,!D.1', '?f.0,?g.0,!F.0,!G.0'],
    34: ['?e.0,!h.0,!E.0,!d.2,!d.3,!b.2,!c.2'],
}
PHASE_2 = {
    0: ['i0,j0,<e.0,r1,?h.0,!H.0,<h.0,s1,l0,w0'],
    1: ['i1'],
    2: ['?d.2,!f.2,!g.2,!D.2,r2,j1'],
    3: ['k1'],
    4: ['l1,w1'],
    5: ['s2,!b.3,!c.3,?d.3,!f.3,!g.3,!D.3,i2'],
    6: ['j2'],
    7: ['k2'],
    8: ['l2,w2'],
    9: ['r3'],
    10: ['s3,i3'],
    11: ['j3'],
    12: ['k3,l3,w3'],
}
SHORT = {'r': '?b,?c,!e,!B,!C', 's': '?f,?g,!h,!F,!G', 'i': '<a,<b,<c,<d,<f,<g', 'j': '?A,<A,?B,<B,?C,<C,?D,<D,?F,<F,?G,<G',
         'k': '?e,!E,<e,?h,!H,<h', 'l': '?E,<E,?H,<H'}


def kernel(*refs):
    wd = refs[len(refs) - SCRATCH - 1]
    slots, blocks = wd.shape[:2]
    counts = [(slots, 2), (slots, 2), (slots, blocks, 2), (slots, blocks, 2), (slots,), (slots,), (2,), (2,), (blocks, 4), (blocks, 4), (8,), (2, slots), (8,), (2,)]
    pl.run_scoped(lambda *sems: body(*refs, *sems), *[pltpu.SemaphoreType.DMA(c) for c in counts])


def body(x_hbm, ids_hbm, norm_hbm, rw_hbm, rb_hbm, wgu_hbm, bgu_hbm, wd_hbm, bd_hbm, out_hbm, wg, wd, z_v, h_v, wbuf, g_v, gfar, gsend, acc, rs_v, x_v, ostage, bias_v, rwp_v, ids_v, norm_v, rw_v, rb_v, bgu_v, bd_v, wg_s, wg_r, wd_s, wd_r, bias_s, bias_r, hg_s, hg_r, rs_s, rs_r, ld_sem, ld2_sem, in_sem, out_sem):
    tok, d_model = x_hbm.shape
    d_ff = wd_hbm.shape[1]
    groups = 2 * d_ff // COLS
    half_g = groups // 2
    blocks = d_model // COLS
    tm = tok // 2
    top_k = ids_hbm.shape[0]
    me = lax.axis_index('ep')
    core = lax.rem(me, 2)
    col = lax.rem(me // 2, RING)
    row = me // (2 * RING)
    away = 1 - 2 * core
    scope = jax.named_scope

    def dev(dy, dx, flip=0):
        other = 1 - core if flip else core
        return {'ep': (lax.rem(row + dy + RING, RING) * RING + lax.rem(col + dx + RING, RING)) * 2 + other}

    peers = [(2 * s, dc, f) for s, dc in ORDER for f in (0, 1)][1:]
    for dy, dx, f in peers + [(1, 0, 0), (-1, 0, 0)]:
        pl.semaphore_signal(pltpu.get_barrier_semaphore(), 1, device_id=dev(dy, dx, f), device_id_type=MESH)

    def remote(src, dst, ssem, rsem, where):
        return pltpu.make_async_remote_copy(src_ref=src, dst_ref=dst, send_sem=ssem, recv_sem=rsem, device_id=where, device_id_type=MESH)

    def ways(table):
        return {(NAMES.index(m[0]), m[1]): (NAMES.index(m[2]), m[3]) for m in table.split(',')}

    gate_up_way, down_way, first_way = ways(GATE_UP_WAYS), ways(DOWN_WAYS), ways(FIRST_WAYS)
    relayed_slots = [NAMES.index(n) for n in 'eh']

    def target(way):
        if way == 's':
            return dev(0, 0, 1)
        return dev(2, 0) if way == 'y' else dev(0, 1 if way == '+' else -1)

    def gate_up(q, ch):
        static = isinstance(q, int)
        src, way = gate_up_way.get((q, str(ch)), (q - 1, 's')) if static else (q - 1, 's')
        part = pl.ds(half_g * ch, half_g)
        here = wbuf.at[part] if static and src == 0 else wg.at[src, part]
        return remote(here, wg.at[q, part], wg_s.at[q, ch], wg_r.at[q, ch], target(way))

    def down(q, j):
        def one(half):
            src, way = down_way.get((q, half), (q - 1, 's'))
            if j == 0:
                src, way = first_way.get((q, half), (src, way))
            rows = slice(None) if half == '.' else pl.ds(d_ff // 2 * int(half), d_ff // 2)
            here = wd_hbm.at[0, :, pl.ds(j * COLS, COLS)] if src == 0 else wd.at[src, j, rows]
            at = 0 if half == '.' else int(half)
            return remote(here, wd.at[q, j, rows], wd_s.at[q, j, at], wd_r.at[q, j, at], target(way))

        return [one(half) for half in ('01' if q in relayed_slots else '.')]

    def hidden_send():
        return remote(h_v.at[pl.ds(tok, tok)], h_v.at[pl.ds(0, tok)], hg_s.at[0], hg_r.at[0], dev(away, 0))

    def gates_send():
        return remote(gsend, gfar, hg_s.at[1], hg_r.at[1], dev(away, 0))

    def bias_send(q, where):
        return remote(bias_v.at[0], bias_v.at[q], bias_s.at[q], bias_r.at[q], where)

    def sum_send(j, t):
        return remote(acc.at[lax.rem(j, 2), t], rs_v.at[j, t], rs_s.at[j, t], rs_r.at[j, t], dev(-away, 0))

    def last_sum_send(i):
        j, t, rows = blocks - 1, i // 2, pl.ds(pl.multiple_of(tm // 2 * lax.rem(i, 2), tm // 2), tm // 2)
        return remote(acc.at[j % 2, t, rows], rs_v.at[j, t, rows], rs_s.at[j, i], rs_r.at[j, i], dev(-away, 0))

    raw = h_v.at[pl.ds(tok, tok)]
    ins = [(wgu_hbm.at[0], raw.at[pl.ds(0, d_model)]), (bgu_hbm, bgu_v), (bd_hbm, bd_v), (x_hbm, x_v), (rw_hbm, rw_v), (rb_hbm, rb_v), (ids_hbm, ids_v), (norm_hbm, norm_v)]
    loads = [pltpu.make_async_copy(src, dst, in_sem.at[i]) for i, (src, dst) in enumerate(ins)]
    for load in loads:
        load.start()
    ri = lax.broadcasted_iota(jnp.int32, (COLS, COLS), 0)
    ci = lax.broadcasted_iota(jnp.int32, (COLS, COLS), 1)
    split = jnp.where(ri == jnp.where(ci < COLS // 2, 2 * ci, 2 * ci - (COLS - 1)), 1.0, 0.0).astype(BF16)
    for load in loads[1:3]:
        load.wait()
    for g in range(groups):
        b = jnp.dot(jnp.broadcast_to(bgu_v[:, COLS * g:COLS * (g + 1)], (16, COLS)), split, preferred_element_type=F32)
        bias_v[0, 2 * g:2 * g + 1, :] = b[0:1, :128]
        bias_v[0, 2 * g + 1:2 * g + 2, :] = b[0:1, 128:]
    for i in range(d_model // 128):
        bias_v[0, 2 * groups + i:2 * groups + i + 1, :] = bd_v[:, 128 * i:128 * (i + 1)].astype(F32)
    with scope('load_w'):
        loads[0].wait()
    for g in range(groups):
        wbuf[g] = jnp.dot(raw[pl.ds(0, d_model), COLS * g:COLS * (g + 1)], split, preferred_element_type=F32).astype(BF16)
    with scope('barrier'):
        pl.semaphore_wait(pltpu.get_barrier_semaphore(), len(peers) + 2)
    bias_msgs = []
    for s, dc in ORDER:
        for f in (0, 1):
            q = 2 * ORDER.index((s, (RING - dc) % RING)) + f
            if q:
                bias_msgs.append(bias_send(q, dev(2 * s, dc, f)))
                bias_msgs[-1].start()
    for name in 'b1,c0,b0,c1,A0,A1'.split(','):
        gate_up(NAMES.index(name[0]), int(name[1])).start()

    def expert_of(shape, dim):
        lane = lax.broadcasted_iota(jnp.int32, shape, dim)
        slot = lane & (SLOTS - 1)
        class_row = jnp.where(lane < SLOTS, row, row + away + RING)
        far = jnp.zeros_like(lane)
        side = jnp.zeros_like(lane)
        for m, (s, dc) in enumerate(ORDER):
            far = jnp.where(slot // 2 == m, 2 * s, far)
            side = jnp.where(slot // 2 == m, dc, side)
        expert = (((class_row + far) & (RING - 1)) * RING + ((col + side) & (RING - 1))) * 2 + jnp.where((slot & 1) == 1, 1 - core, core)
        return jnp.where(lane < 2 * SLOTS, expert, -1)

    for load in loads[3:]:
        load.wait()
    n_exp = rw_v.shape[0]
    transposed = (((1,), (1,)), ((), ()))
    pick = jnp.where(expert_of((128, n_exp), 0) == lax.broadcasted_iota(jnp.int32, (128, n_exp), 1), 1.0, 0.0).astype(BF16)
    rwp_v[...] = jnp.dot(pick, rw_v[...], preferred_element_type=F32).astype(BF16)
    rb_p = lax.dot_general(jnp.broadcast_to(rb_v[...], (16, n_exp)), pick, transposed, preferred_element_type=F32)[0:1]
    expert = expert_of((1, 128), 1).astype(F32)
    norm = jnp.concatenate([norm_v[i:i + 1, :].astype(F32) for i in range(d_model // 128)], axis=1)
    tn = tok // 4

    for i in range(4):
        rows = pl.ds(i * tn, tn)
        own = pl.ds(tok + i * tn, tn)
        xf = x_v[rows, :].astype(F32)
        inv = lax.rsqrt(jnp.mean(xf * xf, axis=-1, keepdims=True) + EPSILON)
        hidden = (xf * inv * norm).astype(BF16)
        h_v[own, :] = hidden
    hidden_send().start()
    for i in range(4):
        rows = pl.ds(i * tn, tn)
        own = pl.ds(tok + i * tn, tn)
        logits = lax.dot_general(h_v[own, :], rwp_v[...], transposed, preferred_element_type=F32) + rb_p
        ids = ids_v[:, i * tn:(i + 1) * tn].astype(F32).T
        chosen = ids[:, 0:1] == expert
        for e in range(1, top_k):
            chosen = chosen | (ids[:, e:e + 1] == expert)
        top = jnp.max(jnp.where(chosen, logits, -jnp.inf), axis=-1, keepdims=True)
        weight = jnp.where(chosen, jnp.exp(logits - top), 0.0)
        gates = weight / jnp.sum(weight, axis=-1, keepdims=True)
        g_v[own, :] = gates
        gsend[:, i * tn:(i + 1) * tn] = gates.T[SLOTS:2 * SLOTS]
    gates_send().start()
    for j in range(blocks):
        for msg in down(1, j):
            msg.start()

    codes = [2 * NAMES.index(n) + int(ch) for n, ch in zip(STEPS[::2], STEPS[1::2])]
    steps = len(codes)
    per, bits = 6, 5
    words = [sum(c << bits * i for i, c in enumerate(codes[at:at + per])) for at in range(0, steps, per)]

    def step_of(s):
        word = jnp.int32(words[0])
        for i, w in enumerate(words[1:]):
            word = jnp.where(s >= per * (i + 1), w, word)
        code = lax.shift_right_logical(word, bits * lax.rem(s, per)) & ((1 << bits) - 1)
        return code // 2, lax.rem(code, 2)

    def buffer_of(s, q, ch):
        return jnp.where(q == 0, ch, 2 + lax.rem(s, 6))

    def weights_load(s):
        q, ch = step_of(s)
        b = buffer_of(s, q, ch)
        return pltpu.make_async_copy(wg.at[q, pl.ds(half_g * ch, half_g)], wbuf.at[pl.ds(half_g * b, half_g)], ld_sem.at[b])

    def down_load(j, q):
        spot = wbuf.at[SLOTS // 2 * (j % 2) + q // 2, pl.ds(d_ff * (q % 2), d_ff)]
        src = wd_hbm.at[0, :, pl.ds(j * COLS, COLS)] if q == 0 else wd.at[q, j]
        return pltpu.make_async_copy(src, spot, ld2_sem.at[j % 2, q])

    def act(text):
        for word in text.split(','):
            what, name, rest = word[0], word[1:2], word[2:]
            if what == '~':
                hidden_send().wait_send()
            elif name == '~':
                hidden_send().wait_recv()
            elif what == 'w':
                for q in range(SLOTS):
                    down_load(int(name), q).wait()
            elif what in SHORT:
                if int(name) < blocks:
                    act(','.join(w + '.' + name for w in SHORT[what].split(',')))
            elif rest[0] != '.':
                msg = gate_up(NAMES.index(name), int(rest))
                msg.start() if what == '!' else msg.wait_recv()
            elif int(rest[1:]) < blocks:
                q, j = NAMES.index(name), int(rest[1:])
                if what == '<':
                    down_load(j, q).start()
                else:
                    for msg in down(q, j):
                        msg.start() if what == '!' else msg.wait_recv()

    def events(table, now):
        for part in sorted({at // 4 for at in table}):
            @pl.when(now // 4 == part)
            def _(part=part):
                for at, texts in table.items():
                    if at // 4 == part:
                        @pl.when(now == at)
                        def _(at=at, texts=texts):
                            with scope('event_' + str(at)):
                                for text in texts:
                                    act(text)

    with scope('bias_wait'):
        for msg in bias_msgs:
            msg.wait_recv()

    @pl.loop(0, 8 + 2 * (steps - 8))
    def _(i):
        single = i < 8
        s = jnp.where(single, i, 4 + i // 2)
        q, ch = step_of(s)
        first = single | (lax.rem(i, 2) == 0)
        last = single | (lax.rem(i, 2) == 1)
        foreign = jnp.where(single, i // 4, lax.rem(i, 2))

        @pl.when(first & (q > 0))
        def _():
            with scope('load_wait'):
                weights_load(s).wait()

        @pl.when(last & (s < steps - 1))
        def _():
            events(PHASE_1, s)
            q1, ch1 = step_of(s + 1)

            @pl.when((lax.rem(q1, 2) == 1) & ((s < 3) | (s >= 7)))
            def _():
                with scope('sib_wait'):
                    gate_up(q1, ch1).wait_recv()

            @pl.when(q1 > 0)
            def _():
                weights_load(s + 1).start()

        w_at = half_g * buffer_of(s, q, ch)
        bias_at = half_g * 2 * ch
        with scope('up'):
            for t in range(2):
                rows = pl.ds(pl.multiple_of((1 - foreign) * tok + t * tm, tm), tm)
                for g in range(half_g):
                    u = jnp.dot(h_v[rows, :], wbuf[w_at + g], preferred_element_type=F32)
                    a = (u[:, :128] + bias_v[q, pl.ds(bias_at + 2 * g, 1), :]).astype(BF16)
                    l = (u[:, 128:] + bias_v[q, pl.ds(bias_at + 2 * g + 1, 1), :]).astype(BF16)
                    a = jnp.minimum(a, LIMIT).astype(F32)
                    l = jnp.clip(l, -LIMIT, LIMIT).astype(F32)
                    z_v[q, rows, pl.ds(pl.multiple_of(128 * (half_g * ch + g), 128), 128)] = (a * jax.nn.sigmoid(ALPHA * a) * (l + 1.0)).astype(BF16)

    with scope('own_sent'):
        for q in (2, 4, 6, 1):
            for ch in range(2):
                gate_up(q, ch).wait_send()
    with scope('gates_in'):
        gates_send().wait_recv()
        for i in range(4):
            g_v[pl.ds(i * tn, tn), 0:SLOTS] = gfar[:, i * tn:(i + 1) * tn].T

    def out_copy(j, t):
        cols = pl.ds(pl.multiple_of(j * COLS, COLS), COLS)
        return pltpu.make_async_copy(ostage.at[t], out_hbm.at[pl.ds(t * tm, tm), cols], out_sem.at[t])

    def finish(j, t, wait_out):
        cols = pl.ds(pl.multiple_of(j * COLS, COLS), COLS)
        pl.when(wait_out)(lambda: out_copy(j - 1, t).wait())
        total = acc[lax.rem(j, 2), 2 + t] + rs_v[j, t]
        ostage[t] = (x_v[pl.ds(t * tm, tm), cols].astype(F32) + total).astype(BF16)
        out_copy(j, t).start()

    def block_sum(j, rows):
        total = None
        for e in range(SLOTS):
            w = wbuf[SLOTS // 2 * lax.rem(j, 2) + e // 2, d_ff * (e % 2):d_ff * (e % 2 + 1), :]
            y = jnp.dot(z_v[e, rows, :], w, preferred_element_type=F32)
            b = jnp.concatenate([bias_v[e, pl.ds(2 * groups + 2 * j, 1), :], bias_v[e, pl.ds(2 * groups + 2 * j + 1, 1), :]], axis=1)
            y = (y + b).astype(BF16).astype(F32)
            p = g_v[rows, e:e + 1]
            term = jnp.where(p > 0, y * p, 0.0)
            total = term if total is None else total + term
        return total

    final = blocks - 1

    @pl.loop(0, 4 * final)
    def _(i):
        j, t = i // 4, lax.rem(i, 4)

        @pl.when((t < 2) & (j >= 2))
        def _():
            sum_send(j - 2, t).wait_send()

        events({at: texts for at, texts in PHASE_2.items() if at < 4 * final}, i)

        @pl.when((t == 3) & (j >= 1))
        def _():
            with scope('finish'):
                for half in range(2):
                    sum_send(j - 1, half).wait_recv()
                    finish(j - 1, half, j >= 2)

        with scope('down'):
            acc[lax.rem(j, 2), t] = block_sum(j, pl.ds(pl.multiple_of(t * tm, tm), tm))

        @pl.when(t < 2)
        def _():
            sum_send(j, t).start()

    with scope('event_final'):
        for text in PHASE_2.get(4 * final, []):
            act(text)
    for t in range(2):
        if final >= 2:
            sum_send(final - 2, t).wait_send()

    @pl.loop(0, 4)
    def _(i):
        with scope('down_far'):
            acc[final % 2, i // 2, pl.ds(pl.multiple_of(tm // 2 * lax.rem(i, 2), tm // 2), tm // 2)] = block_sum(final, pl.ds(pl.multiple_of(tm // 2 * i, tm // 2), tm // 2))
        last_sum_send(i).start()

    @pl.loop(0, 2)
    def _(t):
        with scope('down_own'):
            acc[final % 2, 2 + t] = block_sum(final, pl.ds(pl.multiple_of(tok + t * tm, tm), tm))

    with scope('last_finish'):
        for t in range(2):
            if final:
                sum_send(final - 1, t).wait_recv()
                finish(final - 1, t, final >= 2)
        for t in range(2):
            for i in range(2):
                last_sum_send(2 * t + i).wait_recv()
            finish(final, t, final >= 1)
        for t in range(2):
            out_copy(final, t).wait()
    with scope('drain'):
        for t in range(2):
            if final:
                sum_send(final - 1, t).wait_send()
        for i in range(4):
            last_sum_send(i).wait_send()
        for q in range(SLOTS):
            for ch in range(2):
                if q not in (0, 1, 2, 4, 6):
                    gate_up(q, ch).wait_send()
            for j in range(blocks if q else 0):
                for msg in down(q, j):
                    msg.wait_send()
        for msg in bias_msgs:
            msg.wait_send()
        gates_send().wait_send()


def solution(mesh):
    rows_spec = P(('dp', 'ep'), None)
    assert mesh.shape['ep'] == 2 * RING * RING

    def local_block(x_in, expert_ids, norm_weight, router_w, router_b, w_gate_up, b_gate_up, w_down, b_down):
        tok, d_model = x_in.shape
        d_ff = w_down.shape[1]
        assert w_gate_up.shape[0] == 1 and tok >= d_model
        groups, blocks, tm = 2 * d_ff // COLS, d_model // COLS, tok // 2
        hbm = pl.BlockSpec(memory_space=pltpu.HBM)
        wide = max(groups * 4, SLOTS * d_ff // d_model * 2)
        out = pl.pallas_call(
            kernel,
            out_shape=(
                jax.ShapeDtypeStruct((tok, d_model), BF16),
                jax.ShapeDtypeStruct((SLOTS, groups, d_model, COLS), BF16),
                jax.ShapeDtypeStruct((SLOTS, blocks, d_ff, COLS), BF16),
            ),
            in_specs=[hbm] * 9,
            out_specs=(hbm, hbm, hbm),
            scratch_shapes=[
                pltpu.VMEM((SLOTS, 2 * tok, d_ff), BF16),
                pltpu.VMEM((2 * tok, d_model), BF16),
                pltpu.VMEM((wide, d_model, COLS), BF16),
                pltpu.VMEM((2 * tok, 128), F32),
                pltpu.VMEM((SLOTS, tok), F32),
                pltpu.VMEM((SLOTS, tok), F32),
                pltpu.VMEM((2, 4, tm, COLS), F32),
                pltpu.VMEM((blocks, 2, tm, COLS), F32),
                pltpu.VMEM((tok, d_model), BF16),
                pltpu.VMEM((2, tm, COLS), BF16),
                pltpu.VMEM((SLOTS, 2 * groups + d_model // 128, 128), F32),
                pltpu.VMEM((128, d_model), BF16),
                pltpu.VMEM(expert_ids.T.shape, jnp.int32),
                pltpu.VMEM((d_model // 128, 128), BF16),
                pltpu.VMEM(router_w.T.shape, BF16),
                pltpu.VMEM(router_b[None].shape, BF16),
                pltpu.VMEM(b_gate_up.shape, BF16),
                pltpu.VMEM(b_down.shape, BF16),
            ],
            compiler_params=pltpu.CompilerParams(collective_id=0, has_side_effects=True, vmem_limit_bytes=67043328),
        )(x_in, expert_ids.T, norm_weight.reshape(-1, 128), router_w.T, router_b[None], w_gate_up, b_gate_up, w_down, b_down)
        return out[0]

    return jax.shard_map(local_block, mesh=mesh, in_specs=(rows_spec, rows_spec, P(), P(), P(), P('ep', None, None), P('ep', None), P('ep', None, None), P('ep', None)), out_specs=rows_spec, check_vma=False)
```

```python
import jax
import jax.numpy as jnp
from jax import lax
from jax.experimental import pallas as pl
from jax.experimental.pallas import tpu as pltpu
from jax.sharding import PartitionSpec as P

EPSILON = 1e-5
LIMIT = 7.0
ALPHA = 1.702
F32, BF16 = jnp.float32, jnp.bfloat16
MESH = pl.DeviceIdType.MESH
COLS = 256
RING = 4
ORDER = [(0, 0), (0, 3), (0, 1), (1, 0), (0, 2), (1, 3), (1, 1), (1, 2)]
SLOTS = 2 * len(ORDER)
SCRATCH = 20
NAMES = 'aAbBcCdDeEfFgGhH'
GATE_UP_WAYS = 'b0a+,b1a+,c0a-,c1a-,d0ay,d1ay,e0c-,e1b+,' + 'f0d+,f1by,g0d-,g1cy,h0g-,h1f+'
DOWN_WAYS = 'b.a+,c.a-,d.ay,e0b+,e1c-,f.d+,g.d-,h0f+,h1g-'
FIRST_WAYS, EARLY = 'h0ey,h1ey', 1
STEPS = 'a0a1A0A1a0a1A0A1b1B1c0C0b0B0c1C1d0D0' + 'e0e1E0E1f1F1f0F0g0G0g1G1h1H1h0H0d1D1'
PHASE_1 = {
    3: ['~,!d0,?~,*'],
    7: ['?b1,?c0,!e1,!e0,!f1,!B1,!C0'],
    11: ['?b0,?c1,!g1,!B0,!C1'],
    13: ['?d0,!f0,!g0,!D0,!d1'],
    17: ['!c.0,?e0,?e1,!E0,!E1,!d.1'],
    21: ['?f1,!h1,!F1,!b.0,!b.1'],
    23: ['?f0,?g0,!h0,!F0,!G0,!c.1'],
    27: ['?g1,!G1,?d.0,!D.0'],
    29: ['?h1,!H1'],
    31: ['?h0,!H0', 'r0,!f.0,!g.0'],
    33: ['?d1,!D1,r1,?d.1,!f.1,!g.1,!D.1', '?e.0,!h.0,!E.0,!d.2,!b.2,!c.2'],
}
PHASE_2 = {
    0: ['?f.0,?g.0,!F.0,!G.0,i0,j0,<e.0', '?h.0,!H.0,<h.0,!d.3,l0,w0'],
    1: ['s1,?d.2,!f.2,!g.2,!D.2,i1'],
    2: ['?e.1,!E.1,j1'],
    3: ['<e.1,?h.1,!H.1,<h.1,r2'],
    4: ['l1'],
    5: ['w1'],
    6: ['s2,!b.3,!c.3,?d.3,!f.3,!g.3,!D.3,i2'],
    7: ['j2'],
    8: ['k2'],
    9: ['l2'],
    10: ['w2'],
    11: ['r3'],
    12: ['s3,i3'],
    13: ['j3'],
    14: ['k3'],
    15: ['l3,w3'],
}
SHORT = {'r': '?b,?c,!e,!B,!C', 's': '?f,?g,!h,!F,!G', 'i': '<a,<b,<c,<d,<f,<g', 'j': '?A,<A,?B,<B,?C,<C,?D,<D,?F,<F,?G,<G',
         'k': '?e,!E,<e,?h,!H,<h', 'l': '?E,<E,?H,<H'}


def kernel(*refs):
    wd = refs[len(refs) - SCRATCH - 1]
    slots, blocks = wd.shape[:2]
    counts = [(slots, 2), (slots, 2), (slots, blocks, 2), (slots, blocks, 2), (slots,), (slots,), (2,), (2,), (blocks, 8), (blocks, 8), (8,), (2, slots), (8,), (2,), (8,)]
    pl.run_scoped(lambda *sems: body(*refs, *sems), *[pltpu.SemaphoreType.DMA(c) for c in counts])


def body(x_hbm, ids_hbm, norm_hbm, rw_hbm, rb_hbm, wgu_hbm, bgu_hbm, wd_hbm, bd_hbm, out_hbm, wg, wd, z_v, h_v, wbuf, g_v, gfar, gsend, acc, rs_v, x_v, ostage, late_v, bias_v, bias_b, rwp_v, ids_v, norm_v, rw_v, rb_v, bgu_v, bd_v, wg_s, wg_r, wd_s, wd_r, bias_s, bias_r, hg_s, hg_r, rs_s, rs_r, ld_sem, ld2_sem, in_sem, out_sem, last_sem):
    tok, d_model = x_hbm.shape
    d_ff = wd_hbm.shape[1]
    groups = 2 * d_ff // COLS
    half_g = groups // 2
    blocks = d_model // COLS
    tm = tok // 2
    top_k = ids_hbm.shape[0]
    me = lax.axis_index('ep')
    core = lax.rem(me, 2)
    col = lax.rem(me // 2, RING)
    row = me // (2 * RING)
    away = 1 - 2 * core
    scope = jax.named_scope

    def dev(dy, dx, flip=0):
        other = 1 - core if flip else core
        return {'ep': (lax.rem(row + dy + RING, RING) * RING + lax.rem(col + dx + RING, RING)) * 2 + other}

    peers = [(2 * s, dc, f) for s, dc in ORDER for f in (0, 1)][1:]
    for dy, dx, f in peers + [(1, 0, 0), (-1, 0, 0)]:
        pl.semaphore_signal(pltpu.get_barrier_semaphore(), 1, device_id=dev(dy, dx, f), device_id_type=MESH)

    def remote(src, dst, ssem, rsem, where):
        return pltpu.make_async_remote_copy(src_ref=src, dst_ref=dst, send_sem=ssem, recv_sem=rsem, device_id=where, device_id_type=MESH)

    def ways(table):
        return {(NAMES.index(m[0]), m[1]): (NAMES.index(m[2]), m[3]) for m in table.split(',')}

    gate_up_way, down_way, first_way = ways(GATE_UP_WAYS), ways(DOWN_WAYS), ways(FIRST_WAYS)
    relayed_slots = [NAMES.index(n) for n in 'eh']
    late_slots = [NAMES.index(n) for n in 'eEhH']

    def target(way):
        if way == 's':
            return dev(0, 0, 1)
        return dev(2, 0) if way == 'y' else dev(0, 1 if way == '+' else -1)

    def gate_up(q, ch):
        static = isinstance(q, int)
        src, way = gate_up_way.get((q, str(ch)), (q - 1, 's')) if static else (q - 1, 's')
        part = pl.ds(half_g * ch, half_g)
        here = wbuf.at[part] if static and src == 0 else wg.at[src, part]
        return remote(here, wg.at[q, part], wg_s.at[q, ch], wg_r.at[q, ch], target(way))

    def place(q, j, rows=slice(None)):
        if j == blocks - 1 and q in late_slots:
            return late_v.at[late_slots.index(q), rows]
        return wd.at[q, j, rows]

    def down(q, j):
        def one(half):
            src, way = down_way.get((q, half), (q - 1, 's'))
            if j < EARLY:
                src, way = first_way.get((q, half), (src, way))
            rows = slice(None) if half == '.' else pl.ds(d_ff // 2 * int(half), d_ff // 2)
            here = wd_hbm.at[0, :, pl.ds(j * COLS, COLS)] if src == 0 else place(src, j, rows)
            at = 0 if half == '.' else int(half)
            return remote(here, place(q, j, rows), wd_s.at[q, j, at], wd_r.at[q, j, at], target(way))

        return [one(half) for half in ('01' if q in relayed_slots else '.')]

    def hidden_send():
        return remote(h_v.at[pl.ds(tok, tok)], h_v.at[pl.ds(0, tok)], hg_s.at[0], hg_r.at[0], dev(away, 0))

    def gates_send():
        return remote(gsend, gfar, hg_s.at[1], hg_r.at[1], dev(away, 0))

    def bias_send(q, where):
        return remote(bias_b.at[0], bias_b.at[q], bias_s.at[q], bias_r.at[q], where)

    def sum_send(j, t):
        return remote(acc.at[lax.rem(j, 2), t], rs_v.at[j, t], rs_s.at[j, t], rs_r.at[j, t], dev(-away, 0))

    pieces = 8
    few = tok // pieces

    def piece(i):
        per_tile = pieces // 2
        return i // per_tile, pl.ds(pl.multiple_of(few * lax.rem(i, per_tile), few), few)

    def last_sum_send(i):
        j, (t, rows) = blocks - 1, piece(i)
        return remote(acc.at[j % 2, t, rows], rs_v.at[j, t, rows], rs_s.at[j, i], rs_r.at[j, i], dev(-away, 0))

    raw = h_v.at[pl.ds(tok, tok)]
    ins = [(wgu_hbm.at[0], raw.at[pl.ds(0, d_model)]), (bgu_hbm, bgu_v), (bd_hbm, bd_v), (x_hbm, x_v), (rw_hbm, rw_v), (rb_hbm, rb_v), (ids_hbm, ids_v), (norm_hbm, norm_v)]
    loads = [pltpu.make_async_copy(src, dst, in_sem.at[i]) for i, (src, dst) in enumerate(ins)]
    for load in loads:
        load.start()
    ri = lax.broadcasted_iota(jnp.int32, (COLS, COLS), 0)
    ci = lax.broadcasted_iota(jnp.int32, (COLS, COLS), 1)
    split = jnp.where(ri == jnp.where(ci < COLS // 2, 2 * ci, 2 * ci - (COLS - 1)), 1.0, 0.0).astype(BF16)
    for load in loads[1:3]:
        load.wait()
    for g in range(groups):
        b = jnp.dot(jnp.broadcast_to(bgu_v[:, COLS * g:COLS * (g + 1)], (16, COLS)), split, preferred_element_type=F32)
        bias_v[0, 2 * g:2 * g + 1, :] = b[0:1, :128]
        bias_v[0, 2 * g + 1:2 * g + 2, :] = b[0:1, 128:]
    for i in range(d_model // 128):
        bias_v[0, 2 * groups + i:2 * groups + i + 1, :] = bd_v[:, 128 * i:128 * (i + 1)].astype(F32)
    bias_b[0] = bias_v[0].astype(BF16)
    loads[0].wait()
    for g in range(groups):
        wbuf[g] = jnp.dot(raw[pl.ds(0, d_model), COLS * g:COLS * (g + 1)], split, preferred_element_type=F32).astype(BF16)
    with scope('barrier'):
        pl.semaphore_wait(pltpu.get_barrier_semaphore(), len(peers) + 2)
    def first_go(names):
        for name in names.split(','):
            gate_up(NAMES.index(name[0]), int(name[1])).start()

    first_go('b1,c0')
    bias_msgs = {}
    for s, dc in ORDER:
        for f in (0, 1):
            q = 2 * ORDER.index((s, (RING - dc) % RING)) + f
            if q:
                bias_msgs[q] = bias_send(q, dev(2 * s, dc, f))
                bias_msgs[q].start()
    down(NAMES.index('d'), 0)[0].start()
    first_go('b0,c1,A0,A1')

    def expert_of(shape, dim):
        lane = lax.broadcasted_iota(jnp.int32, shape, dim)
        slot = lane & (SLOTS - 1)
        class_row = jnp.where(lane < SLOTS, row, row + away + RING)
        far = jnp.zeros_like(lane)
        side = jnp.zeros_like(lane)
        for m, (s, dc) in enumerate(ORDER):
            far = jnp.where(slot // 2 == m, 2 * s, far)
            side = jnp.where(slot // 2 == m, dc, side)
        expert = (((class_row + far) & (RING - 1)) * RING + ((col + side) & (RING - 1))) * 2 + jnp.where((slot & 1) == 1, 1 - core, core)
        return jnp.where(lane < 2 * SLOTS, expert, -1)

    for load in loads[3:]:
        load.wait()
    n_exp = rw_v.shape[0]
    transposed = (((1,), (1,)), ((), ()))
    pick = jnp.where(expert_of((128, n_exp), 0) == lax.broadcasted_iota(jnp.int32, (128, n_exp), 1), 1.0, 0.0).astype(BF16)
    rwp_v[...] = jnp.dot(pick, rw_v[...], preferred_element_type=F32).astype(BF16)
    rb_p = lax.dot_general(jnp.broadcast_to(rb_v[...], (16, n_exp)), pick, transposed, preferred_element_type=F32)[0:1]
    expert = expert_of((1, 128), 1).astype(F32)
    norm = jnp.concatenate([norm_v[i:i + 1, :].astype(F32) for i in range(d_model // 128)], axis=1)
    tn = tok // 4

    for i in range(4):
        rows = pl.ds(i * tn, tn)
        own = pl.ds(tok + i * tn, tn)
        xf = x_v[rows, :].astype(F32)
        inv = lax.rsqrt(jnp.mean(xf * xf, axis=-1, keepdims=True) + EPSILON)
        hidden = (xf * inv * norm).astype(BF16)
        h_v[own, :] = hidden
    hidden_send().start()
    for i in range(4):
        rows = pl.ds(i * tn, tn)
        own = pl.ds(tok + i * tn, tn)
        logits = lax.dot_general(h_v[own, :], rwp_v[...], transposed, preferred_element_type=F32) + rb_p
        ids = ids_v[:, i * tn:(i + 1) * tn].astype(F32).T
        chosen = ids[:, 0:1] == expert
        for e in range(1, top_k):
            chosen = chosen | (ids[:, e:e + 1] == expert)
        top = jnp.max(jnp.where(chosen, logits, -jnp.inf), axis=-1, keepdims=True)
        weight = jnp.where(chosen, jnp.exp(logits - top), 0.0)
        gates = weight / jnp.sum(weight, axis=-1, keepdims=True)
        g_v[own, :] = gates
        gsend[:, i * tn:(i + 1) * tn] = gates.T[SLOTS:2 * SLOTS]
    gates_send().start()
    for j in range(blocks):
        for msg in down(1, j):
            msg.start()

    codes = [2 * NAMES.index(n) + int(ch) for n, ch in zip(STEPS[::2], STEPS[1::2])]
    steps = len(codes)
    per, bits = 6, 5
    words = [sum(c << bits * i for i, c in enumerate(codes[at:at + per])) for at in range(0, steps, per)]

    def step_of(s):
        word = jnp.int32(words[0])
        for i, w in enumerate(words[1:]):
            word = jnp.where(s >= per * (i + 1), w, word)
        code = lax.shift_right_logical(word, bits * lax.rem(s, per)) & ((1 << bits) - 1)
        return code // 2, lax.rem(code, 2)

    def buffer_of(s, q, ch):
        return jnp.where(q == 0, ch, 2 + lax.rem(s, 6))

    def weights_load(s):
        q, ch = step_of(s)
        b = buffer_of(s, q, ch)
        return pltpu.make_async_copy(wg.at[q, pl.ds(half_g * ch, half_g)], wbuf.at[pl.ds(half_g * b, half_g)], ld_sem.at[b])

    def down_load(j, q):
        spot = wbuf.at[SLOTS // 2 * (j % 2) + q // 2, pl.ds(d_ff * (q % 2), d_ff)]
        src = wd_hbm.at[0, :, pl.ds(j * COLS, COLS)] if q == 0 else wd.at[q, j]
        return pltpu.make_async_copy(src, spot, ld2_sem.at[j % 2, q])

    def act(text):
        for word in text.split(','):
            what, name, rest = word[0], word[1:2], word[2:]
            if what == '~':
                hidden_send().wait_send()
            elif what == '*':
                take_biases(range(2, SLOTS))
            elif name == '~':
                hidden_send().wait_recv()
            elif what == 'w':
                for q in range(SLOTS):
                    if int(name) < blocks - 1 or q not in late_slots:
                        down_load(int(name), q).wait()
            elif what in SHORT:
                if int(name) < blocks:
                    act(','.join(w + '.' + name for w in SHORT[what].split(',')))
            elif rest[0] != '.':
                msg = gate_up(NAMES.index(name), int(rest))
                msg.start() if what == '!' else msg.wait_recv()
            elif int(rest[1:]) < blocks:
                q, j = NAMES.index(name), int(rest[1:])
                if what == '<':
                    if j < blocks - 1 or q not in late_slots:
                        down_load(j, q).start()
                else:
                    for msg in down(q, j):
                        msg.start() if what == '!' else msg.wait_recv()

    def events(table, now):
        for part in sorted({at // 4 for at in table}):
            @pl.when(now // 4 == part)
            def _(part=part):
                for at, texts in table.items():
                    if at // 4 == part:
                        @pl.when(now == at)
                        def _(at=at, texts=texts):
                            with scope('event_' + str(at)):
                                for text in texts:
                                    act(text)

    def take_biases(qs):
        for q in qs:
            bias_msgs[q].wait_recv()
            bias_v[q] = bias_b[q].astype(F32)

    with scope('bias_wait'):
        take_biases([1])

    def before_end(s):
        events(PHASE_1, s)
        q, ch = step_of(s + 1)

        @pl.when((lax.rem(q, 2) == 1) & ((s < 3) | (s >= 7)))
        def _():
            with scope('sib_wait'):
                gate_up(q, ch).wait_recv()

        @pl.when(q > 0)
        def _():
            weights_load(s + 1).start()

    def up(s, bases):
        q, ch = step_of(s)
        w_at = half_g * buffer_of(s, q, ch)
        bias_at = half_g * 2 * ch
        with scope('up'):
            for g in range(half_g):
                for base in bases:
                    rows = pl.ds(pl.multiple_of(base, tm), tm)
                    u = jnp.dot(h_v[rows, :], wbuf[w_at + g], preferred_element_type=F32)
                    a = (u[:, :128] + bias_v[q, pl.ds(bias_at + 2 * g, 1), :]).astype(BF16)
                    l = (u[:, 128:] + bias_v[q, pl.ds(bias_at + 2 * g + 1, 1), :]).astype(BF16)
                    a = jnp.minimum(a, LIMIT).astype(F32)
                    l = jnp.clip(l, -LIMIT, LIMIT).astype(F32)
                    z_v[q, rows, pl.ds(pl.multiple_of(128 * (half_g * ch + g), 128), 128)] = (a * jax.nn.sigmoid(ALPHA * a) * (l + 1.0)).astype(BF16)

    merged = steps - 6

    @pl.loop(0, 2 * merged - 8)
    def _(i):
        single = i < 8
        s = jnp.where(single, i, 4 + i // 2)
        q, ch = step_of(s)
        first = single | (lax.rem(i, 2) == 0)
        foreign = jnp.where(single, i // 4, lax.rem(i, 2))

        @pl.when(first & (q > 0))
        def _():
            weights_load(s).wait()

        @pl.when(single | (lax.rem(i, 2) == 1))
        def _():
            before_end(s)

        up(s, [(1 - foreign) * tok + t * tm for t in range(2)])

    @pl.loop(merged, steps)
    def _(s):
        weights_load(s).wait()
        pl.when(s < steps - 1)(lambda: before_end(s))
        up(s, [t * tm for t in range(4)])

    with scope('own_sent'):
        for q in (2, 4, 6, 1):
            for ch in range(2):
                gate_up(q, ch).wait_send()
    with scope('gates_in'):
        gates_send().wait_recv()
        for i in range(4):
            g_v[pl.ds(i * tn, tn), 0:SLOTS] = gfar[:, i * tn:(i + 1) * tn].T

    def out_copy(j, t):
        cols = pl.ds(pl.multiple_of(j * COLS, COLS), COLS)
        return pltpu.make_async_copy(ostage.at[t], out_hbm.at[pl.ds(t * tm, tm), cols], out_sem.at[t])

    def finish(j, t, wait_out):
        cols = pl.ds(pl.multiple_of(j * COLS, COLS), COLS)
        pl.when(wait_out)(lambda: out_copy(j - 1, t).wait())
        total = acc[lax.rem(j, 2), 2 + t] + rs_v[j, t]
        ostage[t] = (x_v[pl.ds(t * tm, tm), cols].astype(F32) + total).astype(BF16)
        out_copy(j, t).start()

    def block_sum(j, rows, last=False):
        total = None
        for e in range(SLOTS):
            w = late_v[late_slots.index(e)] if last and e in late_slots else wbuf[SLOTS // 2 * lax.rem(j, 2) + e // 2, d_ff * (e % 2):d_ff * (e % 2 + 1), :]
            y = jnp.dot(z_v[e, rows, :], w, preferred_element_type=F32)
            b = jnp.concatenate([bias_v[e, pl.ds(2 * groups + 2 * j, 1), :], bias_v[e, pl.ds(2 * groups + 2 * j + 1, 1), :]], axis=1)
            y = (y + b).astype(BF16).astype(F32)
            p = g_v[rows, e:e + 1]
            term = jnp.where(p > 0, y * p, 0.0)
            total = term if total is None else total + term
        return total

    final, per_block = blocks - 1, 5

    @pl.loop(0, per_block * final)
    def _(i):
        j, t = i // per_block, lax.rem(i, per_block)
        par = lax.rem(j, 2)

        @pl.when((t < 2) & (j >= 2))
        def _():
            sum_send(j - 2, t).wait_send()

        events({at: texts for at, texts in PHASE_2.items() if at < per_block * final}, i)

        @pl.when((t == 3) & (j >= 1))
        def _():
            with scope('finish'):
                for half in range(2):
                    sum_send(j - 1, half).wait_recv()
                    finish(j - 1, half, j >= 2)

        @pl.when(t < 3)
        def _():
            with scope('down'):
                acc[par, t] = block_sum(j, pl.ds(pl.multiple_of(t * tm, tm), tm))

        @pl.when(t < 2)
        def _():
            sum_send(j, t).start()

        @pl.when(t >= 3)
        def _():
            at = pl.multiple_of(tm // 2 * (t - 3), tm // 2)
            with scope('down_half'):
                acc[par, 3, pl.ds(at, tm // 2)] = block_sum(j, pl.ds(pl.multiple_of(tok + tm + at, tm // 2), tm // 2))

    with scope('event_final'):
        for text in PHASE_2.get(per_block * final, []):
            act(text)
    for t in range(2):
        if final >= 2:
            sum_send(final - 2, t).wait_send()

    @pl.loop(0, pieces)
    def _(i):
        t, rows = piece(i)
        with scope('down_far'):
            acc[final % 2, t, rows] = block_sum(final, pl.ds(pl.multiple_of(few * i, few), few), True)
        last_sum_send(i).start()

    @pl.loop(0, 2)
    def _(t):
        with scope('down_own'):
            acc[final % 2, 2 + t] = block_sum(final, pl.ds(pl.multiple_of(tok + t * tm, tm), tm), True)

    def last_copy(i):
        t, rows = piece(i)
        return pltpu.make_async_copy(ostage.at[t, rows], out_hbm.at[pl.ds(pl.multiple_of(few * i, few), few), pl.ds(COLS * final, COLS)], last_sem.at[i])

    with scope('last_finish'):
        for t in range(2):
            if final:
                sum_send(final - 1, t).wait_recv()
                finish(final - 1, t, final >= 2)
        if final:
            for t in range(2):
                out_copy(final - 1, t).wait()

        @pl.loop(0, pieces)
        def _(i):
            last_sum_send(i).wait_recv()
            t, rows = piece(i)
            total = acc[final % 2, 2 + t, rows] + rs_v[final, t, rows]
            ostage[t, rows] = (x_v[pl.ds(pl.multiple_of(few * i, few), few), pl.ds(COLS * final, COLS)].astype(F32) + total).astype(BF16)
            last_copy(i).start()

        for i in range(pieces):
            last_copy(i).wait()
    with scope('drain'):
        for t in range(2):
            if final:
                sum_send(final - 1, t).wait_send()
        for i in range(pieces):
            last_sum_send(i).wait_send()
        for q in range(SLOTS):
            for ch in range(2):
                if q not in (0, 1, 2, 4, 6):
                    gate_up(q, ch).wait_send()
            for j in range(blocks if q else 0):
                for msg in down(q, j):
                    msg.wait_send()
        for msg in bias_msgs.values():
            msg.wait_send()
        gates_send().wait_send()


def copy_out(src, dst, buf, in_sem, out_sem):
    chunks, rows = buf.shape[:2]
    loads = [pltpu.make_async_copy(src.at[pl.ds(rows * i, rows)], buf.at[i], in_sem.at[i]) for i in range(chunks)]
    stores = [pltpu.make_async_copy(buf.at[i], dst.at[pl.ds(rows * i, rows)], out_sem.at[i]) for i in range(chunks)]
    for load in loads:
        load.start()
    for load, store in zip(loads, stores):
        load.wait()
        store.start()
    for store in stores:
        store.wait()


def solution(mesh):
    rows_spec = P(('dp', 'ep'), None)
    assert mesh.shape['ep'] == 2 * RING * RING

    def local_block(x_in, expert_ids, norm_weight, router_w, router_b, w_gate_up, b_gate_up, w_down, b_down):
        tok, d_model = x_in.shape
        d_ff = w_down.shape[1]
        assert w_gate_up.shape[0] == 1 and tok >= d_model
        groups, blocks, tm = 2 * d_ff // COLS, d_model // COLS, tok // 2
        hbm = pl.BlockSpec(memory_space=pltpu.HBM)
        wide = max(groups * 4, SLOTS * d_ff // d_model * 2)
        out = pl.pallas_call(
            kernel,
            out_shape=(
                jax.ShapeDtypeStruct((tok, d_model), BF16),
                jax.ShapeDtypeStruct((SLOTS, groups, d_model, COLS), BF16),
                jax.ShapeDtypeStruct((SLOTS, blocks, d_ff, COLS), BF16),
            ),
            in_specs=[hbm] * 9,
            out_specs=(hbm, hbm, hbm),
            scratch_shapes=[
                pltpu.VMEM((SLOTS, 2 * tok, d_ff), BF16),
                pltpu.VMEM((2 * tok, d_model), BF16),
                pltpu.VMEM((wide, d_model, COLS), BF16),
                pltpu.VMEM((2 * tok, 128), F32),
                pltpu.VMEM((SLOTS, tok), F32),
                pltpu.VMEM((SLOTS, tok), F32),
                pltpu.VMEM((2, 4, tm, COLS), F32),
                pltpu.VMEM((blocks, 2, tm, COLS), F32),
                pltpu.VMEM((tok, d_model), BF16),
                pltpu.VMEM((2, tm, COLS), BF16),
                pltpu.VMEM((4, d_ff, COLS), BF16),
                pltpu.VMEM((SLOTS, 2 * groups + d_model // 128, 128), F32),
                pltpu.VMEM((SLOTS, 2 * groups + d_model // 128, 128), BF16),
                pltpu.VMEM((128, d_model), BF16),
                pltpu.VMEM(expert_ids.T.shape, jnp.int32),
                pltpu.VMEM((d_model // 128, 128), BF16),
                pltpu.VMEM(router_w.T.shape, BF16),
                pltpu.VMEM(router_b[None].shape, BF16),
                pltpu.VMEM(b_gate_up.shape, BF16),
                pltpu.VMEM(b_down.shape, BF16),
            ],
            compiler_params=pltpu.CompilerParams(collective_id=0, has_side_effects=True, vmem_limit_bytes=67043328),
        )(x_in, expert_ids.T, norm_weight.reshape(-1, 128), router_w.T, router_b[None], w_gate_up, b_gate_up, w_down, b_down)
        chunks = 8
        return pl.pallas_call(
            copy_out,
            out_shape=jax.ShapeDtypeStruct((tok, d_model), BF16),
            in_specs=[hbm],
            out_specs=hbm,
            scratch_shapes=[pltpu.VMEM((chunks, tok // chunks, d_model), BF16), pltpu.SemaphoreType.DMA((chunks,)), pltpu.SemaphoreType.DMA((chunks,))],
            compiler_params=pltpu.CompilerParams(vmem_limit_bytes=60000000),
        )(out[0])

    return jax.shard_map(local_block, mesh=mesh, in_specs=(rows_spec, rows_spec, P(), P(), P(), P('ep', None, None), P('ep', None), P('ep', None, None), P('ep', None)), out_specs=rows_spec, check_vma=False)
```

```python
import functools
import math

import jax
import jax.numpy as jnp
from jax import lax
from jax.experimental import pallas as pl
from jax.experimental.pallas import tpu as pltpu
from jax.sharding import PartitionSpec as P

EPSILON = 1e-5
LIMIT = 7.0
ALPHA = 1.702
F32, BF16 = jnp.float32, jnp.bfloat16
MESH = pl.DeviceIdType.MESH
COLS = 256
ORDER = [(0, 0), (0, 3), (0, 1), (1, 0), (0, 2), (1, 3), (1, 1), (1, 2)]
SLOTS = 2 * len(ORDER)
SCRATCH = 20
NAMES = 'aAbBcCdDeEfFgGhH'
GATE_UP_WAYS = 'b0a+,b1a+,c0a-,c1a-,d0ay,d1ay,e0c-,e1b+,' + 'f0d+,f1by,g0d-,g1cy,h0g-,h1f+'
DOWN_WAYS = 'b.a+,c.a-,d.ay,e0b+,e1c-,f.d+,g.d-,h0f+,h1g-'
FIRST_WAYS = 'h0ey,h1ey'
SECOND_WAYS = 'h0f+,h1ey,h2ey,h3g-'
STEPS = 'a0a1A0A1a0a1A0A1b1B1c0C0b0B0c1C1d0D0' + 'e0e1E0E1f1F1f0F0g0G0g1G1h1H1h0H0d1D1'
PHASE_1 = {
    3: ['~,!d0,?~,*'],
    7: ['?b1,?c0,!e1,!e0,!f1,!B1,!C0'],
    11: ['?b0,?c1,!g1,!B0,!C1'],
    13: ['?d0,!f0,!g0,!D0,!d1'],
    17: ['!c.0,?e0,?e1,!E0,!E1,!d.1'],
    21: ['?f1,!h1,!F1,!b.0,!b.1'],
    23: ['?f0,?g0,!h0,!F0,!G0,!c.1'],
    27: ['?g1,!G1,?d.0,!D.0'],
    29: ['?h1,!H1'],
    31: ['?h0,!H0', 'r0,!f.0,!g.0'],
    33: ['?d1,!D1,r1,?d.1,!f.1,!g.1,!D.1', '?e.0,!h.0,!E.0,!d.2,!b.2,!c.2'],
}
PHASE_2 = {
    0: ['?f.0,?g.0,!F.0,!G.0,i0,j0,<e.0,?e.1,^h.1,!E.1', '?h.0,!H.0,<h.0,!d.3,l0,w0'],
    1: ['s1,?d.2,!f.2,!g.2,!D.2,i1'],
    2: ['j1'],
    3: ['<e.1,?h.1,!H.1,<h.1,r2'],
    4: ['l1'],
    5: ['w1'],
    6: ['s2,!b.3,!c.3,?d.3,!f.3,!g.3,!D.3,i2'],
    7: ['j2'],
    8: ['k2'],
    9: ['l2'],
    10: ['w2'],
    11: ['r3'],
    12: ['s3,i3'],
    13: ['j3'],
    14: ['k3'],
    15: ['l3,w3'],
}
SHORT = {'r': '?b,?c,!e,!B,!C', 's': '?f,?g,!h,!F,!G', 'i': '<a,<b,<c,<d,<f,<g', 'j': '?A,<A,?B,<B,?C,<C,?D,<D,?F,<F,?G,<G',
         'k': '?e,!E,<e,?h,!H,<h', 'l': '?E,<E,?H,<H'}


def kernel(ring, *refs):
    wd = refs[len(refs) - SCRATCH - 1]
    slots, blocks = wd.shape[:2]
    counts = [(slots, 2), (slots, 2), (slots, blocks, 4), (slots, blocks, 4), (slots,), (slots,), (2,), (2,), (blocks, 8), (blocks, 8), (8,), (2, slots), (8,), (2,), (8,)]
    pl.run_scoped(lambda *sems: body(ring, *refs, *sems), *[pltpu.SemaphoreType.DMA(c) for c in counts])


def body(ring, x_hbm, ids_hbm, norm_hbm, rw_hbm, rb_hbm, wgu_hbm, bgu_hbm, wd_hbm, bd_hbm, out_hbm, wg, wd, z_v, h_v, wbuf, g_v, gfar, gsend, acc, rs_v, x_v, ostage, late_v, bias_v, bias_b, rwp_v, ids_v, norm_v, rw_v, rb_v, bgu_v, bd_v, wg_s, wg_r, wd_s, wd_r, bias_s, bias_r, hg_s, hg_r, rs_s, rs_r, ld_sem, ld2_sem, in_sem, out_sem, last_sem):
    tok, d_model = x_hbm.shape
    d_ff = wd_hbm.shape[1]
    groups = 2 * d_ff // COLS
    half_g = groups // 2
    blocks = d_model // COLS
    tm = tok // 2
    top_k = ids_hbm.shape[0]
    me = lax.axis_index('ep')
    core = lax.rem(me, 2)
    col = lax.rem(me // 2, ring)
    row = me // (2 * ring)
    away = 1 - 2 * core
    scope = jax.named_scope

    def dev(dy, dx, flip=0):
        other = 1 - core if flip else core
        return {'ep': (lax.rem(row + dy + ring, ring) * ring + lax.rem(col + dx + ring, ring)) * 2 + other}

    peers = [(2 * s, dc, f) for s, dc in ORDER for f in (0, 1)][1:]
    for dy, dx, f in peers + [(1, 0, 0), (-1, 0, 0)]:
        pl.semaphore_signal(pltpu.get_barrier_semaphore(), 1, device_id=dev(dy, dx, f), device_id_type=MESH)

    def remote(src, dst, ssem, rsem, where):
        return pltpu.make_async_remote_copy(src_ref=src, dst_ref=dst, send_sem=ssem, recv_sem=rsem, device_id=where, device_id_type=MESH)

    def ways(table):
        return {(NAMES.index(m[0]), m[1]): (NAMES.index(m[2]), m[3]) for m in table.split(',')}

    gate_up_way, down_way = ways(GATE_UP_WAYS), ways(DOWN_WAYS)
    early_ways = [ways(FIRST_WAYS), ways(SECOND_WAYS)]
    relayed_slots = [NAMES.index(n) for n in 'eh']
    late_slots = [NAMES.index(n) for n in 'eEhH']

    def target(way):
        if way == 's':
            return dev(0, 0, 1)
        return dev(2, 0) if way == 'y' else dev(0, 1 if way == '+' else -1)

    def gate_up(q, ch):
        static = isinstance(q, int)
        src, way = gate_up_way.get((q, str(ch)), (q - 1, 's')) if static else (q - 1, 's')
        part = pl.ds(half_g * ch, half_g)
        here = wbuf.at[part] if static and src == 0 else wg.at[src, part]
        return remote(here, wg.at[q, part], wg_s.at[q, ch], wg_r.at[q, ch], target(way))

    def place(q, j, rows=slice(None)):
        if j == blocks - 1 and q in late_slots:
            return late_v.at[late_slots.index(q), rows]
        return wd.at[q, j, rows]

    def down_parts(q, j):
        table = early_ways[j] if j < len(early_ways) and (q, '0') in early_ways[j] else down_way
        parts = [p for p in '0123' if (q, p) in table] or ['.']
        msgs = []
        for at, part in enumerate(parts):
            src, way = table.get((q, part), (q - 1, 's'))
            few = d_ff // len(parts)
            rows = slice(None) if part == '.' else pl.ds(few * at, few)
            here = wd_hbm.at[0, :, pl.ds(j * COLS, COLS)] if src == 0 else place(src, j, rows)
            msgs.append((remote(here, place(q, j, rows), wd_s.at[q, j, at], wd_r.at[q, j, at], target(way)), way))
        return msgs

    def down(q, j):
        return [msg for msg, _ in down_parts(q, j)]

    def hidden_send():
        return remote(h_v.at[pl.ds(tok, tok)], h_v.at[pl.ds(0, tok)], hg_s.at[0], hg_r.at[0], dev(away, 0))

    def gates_send():
        return remote(gsend, gfar, hg_s.at[1], hg_r.at[1], dev(away, 0))

    def bias_send(q, where):
        return remote(bias_b.at[0], bias_b.at[q], bias_s.at[q], bias_r.at[q], where)

    def sum_send(j, t):
        return remote(acc.at[lax.rem(j, 2), t], rs_v.at[j, t], rs_s.at[j, t], rs_r.at[j, t], dev(-away, 0))

    pieces = 8
    few = tok // pieces

    def piece(i):
        per_tile = pieces // 2
        return i // per_tile, pl.ds(pl.multiple_of(few * lax.rem(i, per_tile), few), few)

    def last_sum_send(i):
        j, (t, rows) = blocks - 1, piece(i)
        return remote(acc.at[j % 2, t, rows], rs_v.at[j, t, rows], rs_s.at[j, i], rs_r.at[j, i], dev(-away, 0))

    raw = h_v.at[pl.ds(tok, tok)]
    ins = [(wgu_hbm.at[0], raw.at[pl.ds(0, d_model)]), (bgu_hbm, bgu_v), (bd_hbm, bd_v), (x_hbm, x_v), (rw_hbm, rw_v), (rb_hbm, rb_v), (ids_hbm, ids_v), (norm_hbm, norm_v)]
    loads = [pltpu.make_async_copy(src, dst, in_sem.at[i]) for i, (src, dst) in enumerate(ins)]
    for load in loads:
        load.start()
    ri = lax.broadcasted_iota(jnp.int32, (COLS, COLS), 0)
    ci = lax.broadcasted_iota(jnp.int32, (COLS, COLS), 1)
    split = jnp.where(ri == jnp.where(ci < COLS // 2, 2 * ci, 2 * ci - (COLS - 1)), 1.0, 0.0).astype(BF16)
    for load in loads[1:3]:
        load.wait()
    for g in range(groups):
        b = jnp.dot(jnp.broadcast_to(bgu_v[:, COLS * g:COLS * (g + 1)], (16, COLS)), split, preferred_element_type=F32)
        bias_v[0, 2 * g:2 * g + 1, :] = b[0:1, :128]
        bias_v[0, 2 * g + 1:2 * g + 2, :] = b[0:1, 128:]
    for i in range(d_model // 128):
        bias_v[0, 2 * groups + i:2 * groups + i + 1, :] = bd_v[:, 128 * i:128 * (i + 1)].astype(F32)
    bias_b[0] = bias_v[0].astype(BF16)
    loads[0].wait()
    for g in range(groups):
        wbuf[g] = jnp.dot(raw[pl.ds(0, d_model), COLS * g:COLS * (g + 1)], split, preferred_element_type=F32).astype(BF16)
    with scope('barrier'):
        pl.semaphore_wait(pltpu.get_barrier_semaphore(), len(peers) + 2)
    def first_go(names):
        for name in names.split(','):
            gate_up(NAMES.index(name[0]), int(name[1])).start()

    first_go('b1,c0')
    bias_msgs = {}
    for s, dc in ORDER:
        for f in (0, 1):
            q = 2 * ORDER.index((s, (ring - dc) % ring)) + f
            if q:
                bias_msgs[q] = bias_send(q, dev(2 * s, dc, f))
                bias_msgs[q].start()
    down(NAMES.index('d'), 0)[0].start()
    first_go('b0,c1,A0,A1')

    def expert_of(shape, dim):
        lane = lax.broadcasted_iota(jnp.int32, shape, dim)
        slot = lane & (SLOTS - 1)
        class_row = jnp.where(lane < SLOTS, row, row + away + ring)
        far = jnp.zeros_like(lane)
        side = jnp.zeros_like(lane)
        for m, (s, dc) in enumerate(ORDER):
            far = jnp.where(slot // 2 == m, 2 * s, far)
            side = jnp.where(slot // 2 == m, dc, side)
        expert = (((class_row + far) & (ring - 1)) * ring + ((col + side) & (ring - 1))) * 2 + jnp.where((slot & 1) == 1, 1 - core, core)
        return jnp.where(lane < 2 * SLOTS, expert, -1)

    for load in loads[3:]:
        load.wait()
    n_exp = rw_v.shape[0]
    transposed = (((1,), (1,)), ((), ()))
    pick = jnp.where(expert_of((128, n_exp), 0) == lax.broadcasted_iota(jnp.int32, (128, n_exp), 1), 1.0, 0.0).astype(BF16)
    rwp_v[...] = jnp.dot(pick, rw_v[...], preferred_element_type=F32).astype(BF16)
    rb_p = lax.dot_general(jnp.broadcast_to(rb_v[...], (16, n_exp)), pick, transposed, preferred_element_type=F32)[0:1]
    expert = expert_of((1, 128), 1).astype(F32)
    norm = jnp.concatenate([norm_v[i:i + 1, :].astype(F32) for i in range(d_model // 128)], axis=1)
    tn = tok // 4

    for i in range(4):
        rows = pl.ds(i * tn, tn)
        own = pl.ds(tok + i * tn, tn)
        xf = x_v[rows, :].astype(F32)
        inv = lax.rsqrt(jnp.mean(xf * xf, axis=-1, keepdims=True) + EPSILON)
        hidden = (xf * inv * norm).astype(BF16)
        h_v[own, :] = hidden
    hidden_send().start()
    for i in range(4):
        rows = pl.ds(i * tn, tn)
        own = pl.ds(tok + i * tn, tn)
        logits = lax.dot_general(h_v[own, :], rwp_v[...], transposed, preferred_element_type=F32) + rb_p
        ids = ids_v[:, i * tn:(i + 1) * tn].astype(F32).T
        chosen = ids[:, 0:1] == expert
        for e in range(1, top_k):
            chosen = chosen | (ids[:, e:e + 1] == expert)
        top = jnp.max(jnp.where(chosen, logits, -jnp.inf), axis=-1, keepdims=True)
        weight = jnp.where(chosen, jnp.exp(logits - top), 0.0)
        gates = weight / jnp.sum(weight, axis=-1, keepdims=True)
        g_v[own, :] = gates
        gsend[:, i * tn:(i + 1) * tn] = gates.T[SLOTS:2 * SLOTS]
    gates_send().start()
    for j in range(blocks):
        for msg in down(1, j):
            msg.start()

    codes = [2 * NAMES.index(n) + int(ch) for n, ch in zip(STEPS[::2], STEPS[1::2])]
    steps = len(codes)
    per, bits = 6, 5
    words = [sum(c << bits * i for i, c in enumerate(codes[at:at + per])) for at in range(0, steps, per)]

    def step_of(s):
        word = jnp.int32(words[0])
        for i, w in enumerate(words[1:]):
            word = jnp.where(s >= per * (i + 1), w, word)
        code = lax.shift_right_logical(word, bits * lax.rem(s, per)) & ((1 << bits) - 1)
        return code // 2, lax.rem(code, 2)

    def buffer_of(s, q, ch):
        return jnp.where(q == 0, ch, 2 + lax.rem(s, 6))

    def weights_load(s):
        q, ch = step_of(s)
        b = buffer_of(s, q, ch)
        return pltpu.make_async_copy(wg.at[q, pl.ds(half_g * ch, half_g)], wbuf.at[pl.ds(half_g * b, half_g)], ld_sem.at[b])

    def down_load(j, q):
        spot = wbuf.at[SLOTS // 2 * (j % 2) + q // 2, pl.ds(d_ff * (q % 2), d_ff)]
        src = wd_hbm.at[0, :, pl.ds(j * COLS, COLS)] if q == 0 else wd.at[q, j]
        return pltpu.make_async_copy(src, spot, ld2_sem.at[j % 2, q])

    def act(text):
        for word in text.split(','):
            what, name, rest = word[0], word[1:2], word[2:]
            if what == '~':
                hidden_send().wait_send()
            elif what == '*':
                take_biases(range(2, SLOTS))
            elif name == '~':
                hidden_send().wait_recv()
            elif what == 'w':
                for q in range(SLOTS):
                    if int(name) < blocks - 1 or q not in late_slots:
                        down_load(int(name), q).wait()
            elif what in SHORT:
                if int(name) < blocks:
                    act(','.join(w + '.' + name for w in SHORT[what].split(',')))
            elif rest[0] != '.':
                msg = gate_up(NAMES.index(name), int(rest))
                msg.start() if what == '!' else msg.wait_recv()
            elif int(rest[1:]) < blocks:
                q, j = NAMES.index(name), int(rest[1:])
                if what == '<':
                    if j < blocks - 1 or q not in late_slots:
                        down_load(j, q).start()
                else:
                    mixed = len({way for _, way in down_parts(q, j)} & set('+y')) == 2
                    for msg, way in down_parts(q, j):
                        if what == '?':
                            msg.wait_recv()
                        elif not mixed or (way == 'y') == (what == '^'):
                            msg.start()

    def events(table, now):
        for part in sorted({at // 4 for at in table}):
            @pl.when(now // 4 == part)
            def _(part=part):
                for at, texts in table.items():
                    if at // 4 == part:
                        @pl.when(now == at)
                        def _(at=at, texts=texts):
                            with scope('event_' + str(at)):
                                for text in texts:
                                    act(text)

    def take_biases(qs):
        for q in qs:
            bias_msgs[q].wait_recv()
            bias_v[q] = bias_b[q].astype(F32)

    with scope('bias_wait'):
        take_biases([1])

    def before_end(s):
        events(PHASE_1, s)
        q, ch = step_of(s + 1)

        @pl.when((lax.rem(q, 2) == 1) & ((s < 3) | (s >= 7)))
        def _():
            with scope('sib_wait'):
                gate_up(q, ch).wait_recv()

        @pl.when(q > 0)
        def _():
            weights_load(s + 1).start()

    def up(s, bases):
        q, ch = step_of(s)
        w_at = half_g * buffer_of(s, q, ch)
        bias_at = half_g * 2 * ch
        with scope('up'):
            for g in range(half_g):
                for base in bases:
                    rows = pl.ds(pl.multiple_of(base, tm), tm)
                    u = jnp.dot(h_v[rows, :], wbuf[w_at + g], preferred_element_type=F32)
                    a = (u[:, :128] + bias_v[q, pl.ds(bias_at + 2 * g, 1), :]).astype(BF16)
                    l = (u[:, 128:] + bias_v[q, pl.ds(bias_at + 2 * g + 1, 1), :]).astype(BF16)
                    a = jnp.minimum(a, LIMIT).astype(F32)
                    l = jnp.clip(l, -LIMIT, LIMIT).astype(F32)
                    z_v[q, rows, pl.ds(pl.multiple_of(128 * (half_g * ch + g), 128), 128)] = (a * jax.nn.sigmoid(ALPHA * a) * (l + 1.0)).astype(BF16)

    merged = steps - 6

    @pl.loop(0, 2 * merged - 8)
    def _(i):
        single = i < 8
        s = jnp.where(single, i, 4 + i // 2)
        q, ch = step_of(s)
        first = single | (lax.rem(i, 2) == 0)
        foreign = jnp.where(single, i // 4, lax.rem(i, 2))

        @pl.when(first & (q > 0))
        def _():
            weights_load(s).wait()

        @pl.when(single | (lax.rem(i, 2) == 1))
        def _():
            before_end(s)

        up(s, [(1 - foreign) * tok + t * tm for t in range(2)])

    @pl.loop(merged, steps)
    def _(s):
        weights_load(s).wait()
        pl.when(s < steps - 1)(lambda: before_end(s))
        up(s, [t * tm for t in range(4)])

    with scope('own_sent'):
        for q in (2, 4, 6, 1):
            for ch in range(2):
                gate_up(q, ch).wait_send()
    with scope('gates_in'):
        gates_send().wait_recv()
        for i in range(4):
            g_v[pl.ds(i * tn, tn), 0:SLOTS] = gfar[:, i * tn:(i + 1) * tn].T

    def out_copy(j, t):
        cols = pl.ds(pl.multiple_of(j * COLS, COLS), COLS)
        return pltpu.make_async_copy(ostage.at[t], out_hbm.at[pl.ds(t * tm, tm), cols], out_sem.at[t])

    def finish(j, t, wait_out):
        cols = pl.ds(pl.multiple_of(j * COLS, COLS), COLS)
        pl.when(wait_out)(lambda: out_copy(j - 1, t).wait())
        total = acc[lax.rem(j, 2), 2 + t] + rs_v[j, t]
        ostage[t] = (x_v[pl.ds(t * tm, tm), cols].astype(F32) + total).astype(BF16)
        out_copy(j, t).start()

    def block_sum(j, rows, last=False):
        total = None
        for e in range(SLOTS):
            w = late_v[late_slots.index(e)] if last and e in late_slots else wbuf[SLOTS // 2 * lax.rem(j, 2) + e // 2, d_ff * (e % 2):d_ff * (e % 2 + 1), :]
            y = jnp.dot(z_v[e, rows, :], w, preferred_element_type=F32)
            b = jnp.concatenate([bias_v[e, pl.ds(2 * groups + 2 * j, 1), :], bias_v[e, pl.ds(2 * groups + 2 * j + 1, 1), :]], axis=1)
            y = (y + b).astype(BF16).astype(F32)
            p = g_v[rows, e:e + 1]
            term = jnp.where(p > 0, y * p, 0.0)
            total = term if total is None else total + term
        return total

    final, per_block = blocks - 1, 5

    @pl.loop(0, per_block * final)
    def _(i):
        j, t = i // per_block, lax.rem(i, per_block)
        par = lax.rem(j, 2)

        @pl.when((t < 2) & (j >= 2))
        def _():
            sum_send(j - 2, t).wait_send()

        events({at: texts for at, texts in PHASE_2.items() if at < per_block * final}, i)

        @pl.when((t == 3) & (j >= 1))
        def _():
            with scope('finish'):
                for half in range(2):
                    sum_send(j - 1, half).wait_recv()
                    finish(j - 1, half, j >= 2)

        @pl.when(t < 3)
        def _():
            with scope('down'):
                acc[par, t] = block_sum(j, pl.ds(pl.multiple_of(t * tm, tm), tm))

        @pl.when(t < 2)
        def _():
            sum_send(j, t).start()

        @pl.when(t >= 3)
        def _():
            at = pl.multiple_of(tm // 2 * (t - 3), tm // 2)
            with scope('down_half'):
                acc[par, 3, pl.ds(at, tm // 2)] = block_sum(j, pl.ds(pl.multiple_of(tok + tm + at, tm // 2), tm // 2))

    with scope('event_final'):
        for text in PHASE_2.get(per_block * final, []):
            act(text)
    for t in range(2):
        if final >= 2:
            sum_send(final - 2, t).wait_send()

    @pl.loop(0, pieces)
    def _(i):
        t, rows = piece(i)
        with scope('down_far'):
            acc[final % 2, t, rows] = block_sum(final, pl.ds(pl.multiple_of(few * i, few), few), True)
        last_sum_send(i).start()

    @pl.loop(0, 2)
    def _(t):
        with scope('down_own'):
            acc[final % 2, 2 + t] = block_sum(final, pl.ds(pl.multiple_of(tok + t * tm, tm), tm), True)

    def last_copy(i):
        t, rows = piece(i)
        return pltpu.make_async_copy(ostage.at[t, rows], out_hbm.at[pl.ds(pl.multiple_of(few * i, few), few), pl.ds(COLS * final, COLS)], last_sem.at[i])

    with scope('last_finish'):
        for t in range(2):
            if final:
                sum_send(final - 1, t).wait_recv()
                finish(final - 1, t, final >= 2)
        if final:
            for t in range(2):
                out_copy(final - 1, t).wait()

        @pl.loop(0, pieces)
        def _(i):
            last_sum_send(i).wait_recv()
            t, rows = piece(i)
            total = acc[final % 2, 2 + t, rows] + rs_v[final, t, rows]
            ostage[t, rows] = (x_v[pl.ds(pl.multiple_of(few * i, few), few), pl.ds(COLS * final, COLS)].astype(F32) + total).astype(BF16)
            last_copy(i).start()

        for i in range(pieces):
            last_copy(i).wait()
    with scope('drain'):
        for t in range(2):
            if final:
                sum_send(final - 1, t).wait_send()
        for i in range(pieces):
            last_sum_send(i).wait_send()
        for q in range(SLOTS):
            for ch in range(2):
                if q not in (0, 1, 2, 4, 6):
                    gate_up(q, ch).wait_send()
            for j in range(blocks if q else 0):
                for msg in down(q, j):
                    msg.wait_send()
        for msg in bias_msgs.values():
            msg.wait_send()
        gates_send().wait_send()


def copy_out(src, dst, buf, in_sem, out_sem):
    chunks, rows = buf.shape[:2]
    loads = [pltpu.make_async_copy(src.at[pl.ds(rows * i, rows)], buf.at[i], in_sem.at[i]) for i in range(chunks)]
    stores = [pltpu.make_async_copy(buf.at[i], dst.at[pl.ds(rows * i, rows)], out_sem.at[i]) for i in range(chunks)]
    for load in loads:
        load.start()
    for load, store in zip(loads, stores):
        load.wait()
        store.start()
    for store in stores:
        store.wait()


def solution(mesh):
    rows_spec = P(('dp', 'ep'), None)
    ring = math.isqrt(mesh.shape['ep'] // 2)
    assert 2 * ring * ring == mesh.shape['ep'] == 2 * SLOTS

    def local_block(x_in, expert_ids, norm_weight, router_w, router_b, w_gate_up, b_gate_up, w_down, b_down):
        tok, d_model = x_in.shape
        d_ff = w_down.shape[1]
        assert w_gate_up.shape[0] == 1 and tok >= d_model
        groups, blocks, tm = 2 * d_ff // COLS, d_model // COLS, tok // 2
        hbm = pl.BlockSpec(memory_space=pltpu.HBM)
        wide = max(groups * 4, SLOTS * d_ff // d_model * 2)
        out = pl.pallas_call(
            functools.partial(kernel, ring),
            out_shape=(
                jax.ShapeDtypeStruct((tok, d_model), BF16),
                jax.ShapeDtypeStruct((SLOTS, groups, d_model, COLS), BF16),
                jax.ShapeDtypeStruct((SLOTS, blocks, d_ff, COLS), BF16),
            ),
            in_specs=[hbm] * 9,
            out_specs=(hbm, hbm, hbm),
            scratch_shapes=[
                pltpu.VMEM((SLOTS, 2 * tok, d_ff), BF16),
                pltpu.VMEM((2 * tok, d_model), BF16),
                pltpu.VMEM((wide, d_model, COLS), BF16),
                pltpu.VMEM((2 * tok, 128), F32),
                pltpu.VMEM((SLOTS, tok), F32),
                pltpu.VMEM((SLOTS, tok), F32),
                pltpu.VMEM((2, 4, tm, COLS), F32),
                pltpu.VMEM((blocks, 2, tm, COLS), F32),
                pltpu.VMEM((tok, d_model), BF16),
                pltpu.VMEM((2, tm, COLS), BF16),
                pltpu.VMEM((4, d_ff, COLS), BF16),
                pltpu.VMEM((SLOTS, 2 * groups + d_model // 128, 128), F32),
                pltpu.VMEM((SLOTS, 2 * groups + d_model // 128, 128), BF16),
                pltpu.VMEM((128, d_model), BF16),
                pltpu.VMEM(expert_ids.T.shape, jnp.int32),
                pltpu.VMEM((d_model // 128, 128), BF16),
                pltpu.VMEM(router_w.T.shape, BF16),
                pltpu.VMEM(router_b[None].shape, BF16),
                pltpu.VMEM(b_gate_up.shape, BF16),
                pltpu.VMEM(b_down.shape, BF16),
            ],
            compiler_params=pltpu.CompilerParams(collective_id=0, has_side_effects=True, vmem_limit_bytes=67043328),
        )(x_in, expert_ids.T, norm_weight.reshape(-1, 128), router_w.T, router_b[None], w_gate_up, b_gate_up, w_down, b_down)
        chunks = 8
        return pl.pallas_call(
            copy_out,
            out_shape=jax.ShapeDtypeStruct((tok, d_model), BF16),
            in_specs=[hbm],
            out_specs=hbm,
            scratch_shapes=[pltpu.VMEM((chunks, tok // chunks, d_model), BF16), pltpu.SemaphoreType.DMA((chunks,)), pltpu.SemaphoreType.DMA((chunks,))],
            compiler_params=pltpu.CompilerParams(vmem_limit_bytes=60000000),
        )(out[0])

    return jax.shard_map(local_block, mesh=mesh, in_specs=(rows_spec, rows_spec, P(), P(), P(), P('ep', None, None), P('ep', None), P('ep', None, None), P('ep', None)), out_specs=rows_spec, check_vma=False)
```

```python
import functools
import math

import jax
import jax.numpy as jnp
from jax import lax
from jax.experimental import pallas as pl
from jax.experimental.pallas import tpu as pltpu
from jax.sharding import PartitionSpec as P

EPSILON = 1e-5
LIMIT = 7.0
ALPHA = 1.702
F32, BF16 = jnp.float32, jnp.bfloat16
MESH = pl.DeviceIdType.MESH
COLS = 256
ORDER = [(0, 0), (0, 3), (0, 1), (1, 0), (0, 2), (1, 3), (1, 1), (1, 2)]
SLOTS = 2 * len(ORDER)
SCRATCH = 20
NAMES = 'aAbBcCdDeEfFgGhH'
GATE_UP_WAYS = 'b0a+,b1a+,c0a-,c1a-,d0ay,d1ay,e0c-,e1b+,' + 'f0d+,f1by,g0d-,g1cy,h0g-,h1f+'
DOWN_WAYS = 'b.a+,c.a-,d.ay,e0b+,e1c-,f.d+,g.d-,h0f+,h1g-'
FIRST_WAYS = 'h0ey,h1ey'
SECOND_WAYS = 'h0f+,h1ey,h2ey,h3g-'
STEPS = 'a0a1A0A1a0a1A0A1b1B1c0C0b0B0c1C1d0D0' + 'e0e1E0E1f1F1f0F0g0G0g1G1h1H1h0H0d1D1'
PHASE_1 = {
    3: ['~,!d0,?~,*'],
    7: ['?b1,?c0,!e1,!e0,!f1,!B1,!C0'],
    11: ['?b0,?c1,!g1,!B0,!C1'],
    13: ['?d0,!f0,!g0,!D0,!d1'],
    17: ['!c.0,?e0,?e1,!E0,!E1'],
    21: ['?f1,!h1,!F1,!b.0,!b.1'],
    23: ['?f0,?g0,!h0,!F0,!G0,!c.1'],
    27: ['?g1,!G1,?d.0,!D.0'],
    29: ['?h1,!H1'],
    31: ['?h0,!H0', 'r0,!f.0,!g.0'],
    33: ['?d1,!D1,r1,?d.1,!f.1,!g.1,!D.1', '?e.0,!h.0,!E.0,!d.2,!b.2,!c.2'],
}
PHASE_2 = {
    0: ['?f.0,?g.0,!F.0,!G.0,i0,j0,<e.0,?e.1,^h.1,!E.1', '?h.0,!H.0,<h.0,!d.3,l0,w0'],
    1: ['s1,?d.2,!f.2,!g.2,!D.2,i1'],
    2: ['j1'],
    4: ['<e.1,?h.1,!H.1,<h.1,r2'],
    5: ['l1'],
    6: ['w1'],
    7: ['s2,!b.3,!c.3,?d.3,!f.3,!g.3,!D.3,i2'],
    8: ['j2'],
    10: ['k2'],
    11: ['l2'],
    12: ['w2'],
    13: ['r3'],
    15: ['s3,i3'],
    16: ['j3'],
    17: ['%'],
    18: ['&,w3'],
}
SHORT = {'r': '?b,?c,!e,!B,!C', 's': '?f,?g,!h,!F,!G', 'i': '<a,<b,<c,<d,<f,<g', 'j': '?A,<A,?B,<B,?C,<C,?D,<D,?F,<F,?G,<G',
         'k': '?e,!E,<e,?h,!H,<h', 'l': '?E,<E,?H,<H'}


def kernel(ring, *refs):
    wd = refs[len(refs) - SCRATCH - 1]
    slots, blocks = wd.shape[:2]
    counts = [(slots, 2), (slots, 2), (slots, blocks, 4), (slots, blocks, 4), (slots,), (slots,), (2,), (2,), (blocks, 8), (blocks, 8), (8,), (2, slots), (8,), (2,), (8,)]
    pl.run_scoped(lambda *sems: body(ring, *refs, *sems), *[pltpu.SemaphoreType.DMA(c) for c in counts])


def body(ring, x_hbm, ids_hbm, norm_hbm, rw_hbm, rb_hbm, wgu_hbm, bgu_hbm, wd_hbm, bd_hbm, out_hbm, wg, wd, z_v, h_v, wbuf, g_v, gfar, gsend, acc, rs_v, x_v, ostage, late_v, bias_v, bias_b, rwp_v, ids_v, norm_v, rw_v, rb_v, bgu_v, bd_v, wg_s, wg_r, wd_s, wd_r, bias_s, bias_r, hg_s, hg_r, rs_s, rs_r, ld_sem, ld2_sem, in_sem, out_sem, last_sem):
    tok, d_model = x_hbm.shape
    d_ff = wd_hbm.shape[1]
    groups = 2 * d_ff // COLS
    half_g = groups // 2
    blocks = d_model // COLS
    tm = tok // 2
    top_k = ids_hbm.shape[0]
    me = lax.axis_index('ep')
    core = lax.rem(me, 2)
    col = lax.rem(me // 2, ring)
    row = me // (2 * ring)
    away = 1 - 2 * core
    scope = jax.named_scope

    def dev(dy, dx, flip=0):
        other = 1 - core if flip else core
        return {'ep': (lax.rem(row + dy + ring, ring) * ring + lax.rem(col + dx + ring, ring)) * 2 + other}

    peers = [(2 * s, dc, f) for s, dc in ORDER for f in (0, 1)][1:]
    for dy, dx, f in peers + [(1, 0, 0), (-1, 0, 0)]:
        pl.semaphore_signal(pltpu.get_barrier_semaphore(), 1, device_id=dev(dy, dx, f), device_id_type=MESH)

    def remote(src, dst, ssem, rsem, where):
        return pltpu.make_async_remote_copy(src_ref=src, dst_ref=dst, send_sem=ssem, recv_sem=rsem, device_id=where, device_id_type=MESH)

    def ways(table):
        return {(NAMES.index(m[0]), m[1]): (NAMES.index(m[2]), m[3]) for m in table.split(',')}

    gate_up_way, down_way = ways(GATE_UP_WAYS), ways(DOWN_WAYS)
    early_ways = [ways(FIRST_WAYS), ways(SECOND_WAYS)]
    relayed_slots = [NAMES.index(n) for n in 'eh']
    late_slots = [NAMES.index(n) for n in 'eEhH']

    def target(way):
        if way == 's':
            return dev(0, 0, 1)
        return dev(2, 0) if way == 'y' else dev(0, 1 if way == '+' else -1)

    def gate_up(q, ch):
        static = isinstance(q, int)
        src, way = gate_up_way.get((q, str(ch)), (q - 1, 's')) if static else (q - 1, 's')
        part = pl.ds(half_g * ch, half_g)
        here = wbuf.at[part] if static and src == 0 else wg.at[src, part]
        return remote(here, wg.at[q, part], wg_s.at[q, ch], wg_r.at[q, ch], target(way))

    def place(q, j, rows=slice(None)):
        if j == blocks - 1 and q in late_slots:
            return late_v.at[late_slots.index(q), rows]
        return wd.at[q, j, rows]

    def down_ways(q, j):
        table = early_ways[j] if j < len(early_ways) and (q, '0') in early_ways[j] else down_way
        parts = [p for p in '0123' if (q, p) in table]
        return [table[q, p] for p in parts] if parts else [table.get((q, '.'), (q - 1, 's'))]

    def down(q, j, wanted='s+-y'):
        parts = down_ways(q, j)
        few = d_ff // len(parts)
        msgs = []
        for at, (src, way) in enumerate(parts):
            if way in wanted:
                rows = pl.ds(few * at, few)
                here = wd_hbm.at[0, rows, pl.ds(j * COLS, COLS)] if src == 0 else place(src, j, rows)
                there, slot, where = place(q, j, rows), q, target(way)
                if j == blocks - 1 and q in relayed_slots:
                    slot = q + 1 - core
                    there = late_v.at[late_slots.index(q) + 1 - core, rows]
                    where = {'ep': where['ep'] + 1 - core}
                msgs.append(remote(here, there, wd_s.at[q, j, at], wd_r.at[slot, j, at], where))
        return msgs

    def late_landed(q):
        for half in range(2):
            rows = pl.ds(d_ff // 2 * half, d_ff // 2)
            spot = late_v.at[late_slots.index(q), rows]
            remote(spot, spot, wd_s.at[q, blocks - 1, half], wd_r.at[q, blocks - 1, half], dev(0, 1)).wait_recv()

    def late_handed(q):
        at, other = late_slots.index(q), late_slots.index(q) ^ 1
        return remote(late_v.at[at], late_v.at[other], wd_s.at[q, blocks - 1, 2], wd_r.at[q ^ 1, blocks - 1, 2], dev(0, 0, 1))

    def hand_on(slots):
        @pl.when(core == 1)
        def _():
            for q in slots:
                late_landed(q)
                late_handed(q).start()

    def take_late():
        @pl.when(core == 0)
        def _():
            for q in late_slots:
                late_handed(q ^ 1).wait_recv()

    def hidden_send():
        return remote(h_v.at[pl.ds(tok, tok)], h_v.at[pl.ds(0, tok)], hg_s.at[0], hg_r.at[0], dev(away, 0))

    def gates_send():
        return remote(gsend, gfar, hg_s.at[1], hg_r.at[1], dev(away, 0))

    def bias_send(q, where):
        return remote(bias_b.at[0], bias_b.at[q], bias_s.at[q], bias_r.at[q], where)

    def sum_send(j, t):
        return remote(acc.at[lax.rem(j, 2), t], rs_v.at[j, t], rs_s.at[j, t], rs_r.at[j, t], dev(-away, 0))

    pieces = 8
    few = tok // pieces

    def piece(i):
        per_tile = pieces // 2
        return i // per_tile, pl.ds(pl.multiple_of(few * lax.rem(i, per_tile), few), few)

    def last_sum_send(i):
        j, (t, rows) = blocks - 1, piece(i)
        return remote(acc.at[j % 2, t, rows], rs_v.at[j, t, rows], rs_s.at[j, i], rs_r.at[j, i], dev(-away, 0))

    raw = h_v.at[pl.ds(tok, tok)]
    ins = [(wgu_hbm.at[0], raw.at[pl.ds(0, d_model)]), (bgu_hbm, bgu_v), (bd_hbm, bd_v), (x_hbm, x_v), (rw_hbm, rw_v), (rb_hbm, rb_v), (ids_hbm, ids_v), (norm_hbm, norm_v)]
    loads = [pltpu.make_async_copy(src, dst, in_sem.at[i]) for i, (src, dst) in enumerate(ins)]
    for load in loads:
        load.start()
    ri = lax.broadcasted_iota(jnp.int32, (COLS, COLS), 0)
    ci = lax.broadcasted_iota(jnp.int32, (COLS, COLS), 1)
    split = jnp.where(ri == jnp.where(ci < COLS // 2, 2 * ci, 2 * ci - (COLS - 1)), 1.0, 0.0).astype(BF16)
    loads[0].wait()
    for g in range(groups):
        wbuf[g] = jnp.dot(raw[pl.ds(0, d_model), COLS * g:COLS * (g + 1)], split, preferred_element_type=F32).astype(BF16)
    with scope('barrier'):
        pl.semaphore_wait(pltpu.get_barrier_semaphore(), len(peers) + 2)
    def first_go(names):
        for name in names.split(','):
            gate_up(NAMES.index(name[0]), int(name[1])).start()

    first_go('b1,c0')
    for load in loads[1:3]:
        load.wait()
    for g in range(groups):
        b = jnp.dot(jnp.broadcast_to(bgu_v[:, COLS * g:COLS * (g + 1)], (16, COLS)), split, preferred_element_type=F32)
        bias_v[0, 2 * g:2 * g + 1, :] = b[0:1, :128]
        bias_v[0, 2 * g + 1:2 * g + 2, :] = b[0:1, 128:]
    for i in range(d_model // 128):
        bias_v[0, 2 * groups + i:2 * groups + i + 1, :] = bd_v[:, 128 * i:128 * (i + 1)].astype(F32)
    bias_b[0] = bias_v[0].astype(BF16)
    bias_msgs = {}
    for s, dc in ORDER:
        for f in (0, 1):
            q = 2 * ORDER.index((s, (ring - dc) % ring)) + f
            if q:
                bias_msgs[q] = bias_send(q, dev(2 * s, dc, f))
                bias_msgs[q].start()
    for j in range(2):
        down(NAMES.index('d'), j)[0].start()
    first_go('b0,c1,A0,A1')

    def expert_of(shape, dim):
        lane = lax.broadcasted_iota(jnp.int32, shape, dim)
        slot = lane & (SLOTS - 1)
        class_row = jnp.where(lane < SLOTS, row, row + away + ring)
        far = jnp.zeros_like(lane)
        side = jnp.zeros_like(lane)
        for m, (s, dc) in enumerate(ORDER):
            far = jnp.where(slot // 2 == m, 2 * s, far)
            side = jnp.where(slot // 2 == m, dc, side)
        expert = (((class_row + far) & (ring - 1)) * ring + ((col + side) & (ring - 1))) * 2 + jnp.where((slot & 1) == 1, 1 - core, core)
        return jnp.where(lane < 2 * SLOTS, expert, -1)

    for load in loads[3:]:
        load.wait()
    n_exp = rw_v.shape[0]
    transposed = (((1,), (1,)), ((), ()))
    pick = jnp.where(expert_of((128, n_exp), 0) == lax.broadcasted_iota(jnp.int32, (128, n_exp), 1), 1.0, 0.0).astype(BF16)
    rwp_v[...] = jnp.dot(pick, rw_v[...], preferred_element_type=F32).astype(BF16)
    rb_p = lax.dot_general(jnp.broadcast_to(rb_v[...], (16, n_exp)), pick, transposed, preferred_element_type=F32)[0:1]
    expert = expert_of((1, 128), 1).astype(F32)
    norm = jnp.concatenate([norm_v[i:i + 1, :].astype(F32) for i in range(d_model // 128)], axis=1)
    tn = tok // 4

    for i in range(4):
        rows = pl.ds(i * tn, tn)
        own = pl.ds(tok + i * tn, tn)
        xf = x_v[rows, :].astype(F32)
        inv = lax.rsqrt(jnp.mean(xf * xf, axis=-1, keepdims=True) + EPSILON)
        hidden = (xf * inv * norm).astype(BF16)
        h_v[own, :] = hidden
    hidden_send().start()
    for i in range(4):
        rows = pl.ds(i * tn, tn)
        own = pl.ds(tok + i * tn, tn)
        logits = lax.dot_general(h_v[own, :], rwp_v[...], transposed, preferred_element_type=F32) + rb_p
        ids = ids_v[:, i * tn:(i + 1) * tn].astype(F32).T
        chosen = ids[:, 0:1] == expert
        for e in range(1, top_k):
            chosen = chosen | (ids[:, e:e + 1] == expert)
        top = jnp.max(jnp.where(chosen, logits, -jnp.inf), axis=-1, keepdims=True)
        weight = jnp.where(chosen, jnp.exp(logits - top), 0.0)
        gates = weight / jnp.sum(weight, axis=-1, keepdims=True)
        g_v[own, :] = gates
        gsend[:, i * tn:(i + 1) * tn] = gates.T[SLOTS:2 * SLOTS]
    gates_send().start()
    for j in range(blocks):
        for msg in down(1, j):
            msg.start()

    codes = [2 * NAMES.index(n) + int(ch) for n, ch in zip(STEPS[::2], STEPS[1::2])]
    steps = len(codes)
    per, bits = 6, 5
    words = [sum(c << bits * i for i, c in enumerate(codes[at:at + per])) for at in range(0, steps, per)]

    def step_of(s):
        word = jnp.int32(words[0])
        for i, w in enumerate(words[1:]):
            word = jnp.where(s >= per * (i + 1), w, word)
        code = lax.shift_right_logical(word, bits * lax.rem(s, per)) & ((1 << bits) - 1)
        return code // 2, lax.rem(code, 2)

    def buffer_of(s, q, ch):
        return jnp.where(q == 0, ch, 2 + lax.rem(s, 6))

    def weights_load(s):
        q, ch = step_of(s)
        b = buffer_of(s, q, ch)
        return pltpu.make_async_copy(wg.at[q, pl.ds(half_g * ch, half_g)], wbuf.at[pl.ds(half_g * b, half_g)], ld_sem.at[b])

    def down_load(j, q):
        spot = wbuf.at[SLOTS // 2 * (j % 2) + q // 2, pl.ds(d_ff * (q % 2), d_ff)]
        src = wd_hbm.at[0, :, pl.ds(j * COLS, COLS)] if q == 0 else wd.at[q, j]
        return pltpu.make_async_copy(src, spot, ld2_sem.at[j % 2, q])

    def act(text):
        for word in text.split(','):
            what, name, rest = word[0], word[1:2], word[2:]
            if what == '~':
                hidden_send().wait_send()
            elif what == '*':
                take_biases(range(2, SLOTS))
            elif name == '~':
                hidden_send().wait_recv()
            elif what == '%':
                hand_on(relayed_slots)
            elif what == '&':
                hand_on([q + 1 for q in relayed_slots])
                take_late()
            elif what == 'w':
                for q in range(SLOTS):
                    if int(name) < blocks - 1 or q not in late_slots:
                        down_load(int(name), q).wait()
            elif what in SHORT:
                if int(name) < blocks:
                    act(','.join(w + '.' + name for w in SHORT[what].split(',')))
            elif rest[0] != '.':
                msg = gate_up(NAMES.index(name), int(rest))
                msg.start() if what == '!' else msg.wait_recv()
            elif int(rest[1:]) < blocks:
                q, j = NAMES.index(name), int(rest[1:])
                if what == '<':
                    if j < blocks - 1 or q not in late_slots:
                        down_load(j, q).start()
                else:
                    mixed = len({way for _, way in down_ways(q, j)}) == 3
                    for msg in down(q, j, {'?': 's+-y', '!': '+-' if mixed else 's+-y', '^': 'y'}[what]):
                        msg.wait_recv() if what == '?' else msg.start()

    def events(table, now):
        for part in sorted({at // 4 for at in table}):
            @pl.when(now // 4 == part)
            def _(part=part):
                for at, texts in table.items():
                    if at // 4 == part:
                        @pl.when(now == at)
                        def _(at=at, texts=texts):
                            with scope('event_' + str(at)):
                                for text in texts:
                                    act(text)

    def take_biases(qs):
        for q in qs:
            bias_msgs[q].wait_recv()
            bias_v[q] = bias_b[q].astype(F32)

    with scope('bias_wait'):
        take_biases([1])

    def before_end(s):
        events(PHASE_1, s)
        q, ch = step_of(s + 1)

        @pl.when((lax.rem(q, 2) == 1) & ((s < 3) | (s >= 7)))
        def _():
            with scope('sib_wait'):
                gate_up(q, ch).wait_recv()

        @pl.when(q > 0)
        def _():
            weights_load(s + 1).start()

    def up(s, bases):
        q, ch = step_of(s)
        w_at = half_g * buffer_of(s, q, ch)
        bias_at = half_g * 2 * ch
        with scope('up'):
            for g in range(half_g):
                for base in bases:
                    rows = pl.ds(pl.multiple_of(base, tm), tm)
                    u = jnp.dot(h_v[rows, :], wbuf[w_at + g], preferred_element_type=F32)
                    a = (u[:, :128] + bias_v[q, pl.ds(bias_at + 2 * g, 1), :]).astype(BF16)
                    l = (u[:, 128:] + bias_v[q, pl.ds(bias_at + 2 * g + 1, 1), :]).astype(BF16)
                    a = jnp.minimum(a, LIMIT).astype(F32)
                    l = jnp.clip(l, -LIMIT, LIMIT).astype(F32)
                    z_v[q, rows, pl.ds(pl.multiple_of(128 * (half_g * ch + g), 128), 128)] = (a * jax.nn.sigmoid(ALPHA * a) * (l + 1.0)).astype(BF16)

    merged = steps - 6

    @pl.loop(0, 2 * merged - 8)
    def _(i):
        single = i < 8
        s = jnp.where(single, i, 4 + i // 2)
        q, ch = step_of(s)
        first = single | (lax.rem(i, 2) == 0)
        foreign = jnp.where(single, i // 4, lax.rem(i, 2))

        @pl.when(first & (q > 0))
        def _():
            weights_load(s).wait()

        @pl.when(single | (lax.rem(i, 2) == 1))
        def _():
            before_end(s)

        up(s, [(1 - foreign) * tok + t * tm for t in range(2)])

    @pl.loop(merged, steps)
    def _(s):
        weights_load(s).wait()
        pl.when(s < steps - 1)(lambda: before_end(s))
        up(s, [t * tm for t in range(4)])

    with scope('own_sent'):
        for q in (2, 4, 6, 1):
            for ch in range(2):
                gate_up(q, ch).wait_send()
    with scope('gates_in'):
        gates_send().wait_recv()
        for i in range(4):
            g_v[pl.ds(i * tn, tn), 0:SLOTS] = gfar[:, i * tn:(i + 1) * tn].T

    def out_copy(j, t):
        cols = pl.ds(pl.multiple_of(j * COLS, COLS), COLS)
        return pltpu.make_async_copy(ostage.at[t], out_hbm.at[pl.ds(t * tm, tm), cols], out_sem.at[t])

    def finish(j, t, wait_out):
        cols = pl.ds(pl.multiple_of(j * COLS, COLS), COLS)
        pl.when(wait_out)(lambda: out_copy(j - 1, t).wait())
        total = acc[lax.rem(j, 2), 2 + t] + rs_v[j, t]
        ostage[t] = (x_v[pl.ds(t * tm, tm), cols].astype(F32) + total).astype(BF16)
        out_copy(j, t).start()

    def block_sum(j, rows, last=False):
        total = None
        for e in range(SLOTS):
            w = late_v[late_slots.index(e)] if last and e in late_slots else wbuf[SLOTS // 2 * lax.rem(j, 2) + e // 2, d_ff * (e % 2):d_ff * (e % 2 + 1), :]
            y = jnp.dot(z_v[e, rows, :], w, preferred_element_type=F32)
            b = jnp.concatenate([bias_v[e, pl.ds(2 * groups + 2 * j, 1), :], bias_v[e, pl.ds(2 * groups + 2 * j + 1, 1), :]], axis=1)
            y = (y + b).astype(BF16).astype(F32)
            p = g_v[rows, e:e + 1]
            term = jnp.where(p > 0, y * p, 0.0)
            total = term if total is None else total + term
        return total

    final, per_block = blocks - 1, 6

    @pl.loop(0, per_block * final)
    def _(i):
        j, t = i // per_block, lax.rem(i, per_block)
        par = lax.rem(j, 2)

        @pl.when((t < 2) & (j >= 2))
        def _():
            sum_send(j - 2, t).wait_send()

        events({at: texts for at, texts in PHASE_2.items() if at < per_block * final}, i)

        @pl.when((t == 4) & (j >= 1))
        def _():
            with scope('finish'):
                for half in range(2):
                    sum_send(j - 1, half).wait_recv()
                    finish(j - 1, half, j >= 2)

        @pl.when(t < 2)
        def _():
            with scope('down'):
                acc[par, t] = block_sum(j, pl.ds(pl.multiple_of(t * tm, tm), tm))

        @pl.when(t < 2)
        def _():
            sum_send(j, t).start()

        @pl.when(t >= 2)
        def _():
            at = pl.multiple_of(tm // 2 * lax.rem(t, 2), tm // 2)
            with scope('down_half'):
                acc[par, 1 + t // 2, pl.ds(at, tm // 2)] = block_sum(j, pl.ds(pl.multiple_of(tok + tm * (t // 2 - 1) + at, tm // 2), tm // 2))

    with scope('event_final'):
        for text in PHASE_2.get(per_block * final, []):
            act(text)
    for t in range(2):
        if final >= 2:
            sum_send(final - 2, t).wait_send()

    @pl.loop(0, pieces)
    def _(i):
        t, rows = piece(i)
        with scope('down_far'):
            acc[final % 2, t, rows] = block_sum(final, pl.ds(pl.multiple_of(few * i, few), few), True)
        last_sum_send(i).start()

    @pl.loop(0, 2)
    def _(t):
        with scope('down_own'):
            acc[final % 2, 2 + t] = block_sum(final, pl.ds(pl.multiple_of(tok + t * tm, tm), tm), True)

    def last_copy(i):
        t, rows = piece(i)
        return pltpu.make_async_copy(ostage.at[t, rows], out_hbm.at[pl.ds(pl.multiple_of(few * i, few), few), pl.ds(COLS * final, COLS)], last_sem.at[i])

    with scope('last_finish'):
        for t in range(2):
            if final:
                sum_send(final - 1, t).wait_recv()
                finish(final - 1, t, final >= 2)
        if final:
            for t in range(2):
                out_copy(final - 1, t).wait()

        @pl.loop(0, pieces)
        def _(i):
            last_sum_send(i).wait_recv()
            t, rows = piece(i)
            total = acc[final % 2, 2 + t, rows] + rs_v[final, t, rows]
            ostage[t, rows] = (x_v[pl.ds(pl.multiple_of(few * i, few), few), pl.ds(COLS * final, COLS)].astype(F32) + total).astype(BF16)
            last_copy(i).start()

        for i in range(pieces):
            last_copy(i).wait()
    with scope('drain'):
        for t in range(2):
            if final:
                sum_send(final - 1, t).wait_send()
        for i in range(pieces):
            last_sum_send(i).wait_send()
        for q in range(SLOTS):
            for ch in range(2):
                if q not in (0, 1, 2, 4, 6):
                    gate_up(q, ch).wait_send()
            for j in range(blocks if q else 0):
                if j < blocks - 1 or q - 1 not in relayed_slots:
                    for msg in down(q, j):
                        msg.wait_send()

        @pl.when(core == 1)
        def _():
            for q in late_slots:
                late_handed(q).wait_send()

        for msg in bias_msgs.values():
            msg.wait_send()
        gates_send().wait_send()


def copy_out(src, dst, buf, in_sem, out_sem):
    chunks, rows = buf.shape[:2]
    loads = [pltpu.make_async_copy(src.at[pl.ds(rows * i, rows)], buf.at[i], in_sem.at[i]) for i in range(chunks)]
    stores = [pltpu.make_async_copy(buf.at[i], dst.at[pl.ds(rows * i, rows)], out_sem.at[i]) for i in range(chunks)]
    for load in loads:
        load.start()
    for load, store in zip(loads, stores):
        load.wait()
        store.start()
    for store in stores:
        store.wait()


def solution(mesh):
    rows_spec = P(('dp', 'ep'), None)
    ring = math.isqrt(mesh.shape['ep'] // 2)
    assert 2 * ring * ring == mesh.shape['ep'] == 2 * SLOTS

    def local_block(x_in, expert_ids, norm_weight, router_w, router_b, w_gate_up, b_gate_up, w_down, b_down):
        tok, d_model = x_in.shape
        d_ff = w_down.shape[1]
        assert w_gate_up.shape[0] == 1 and tok >= d_model
        groups, blocks, tm = 2 * d_ff // COLS, d_model // COLS, tok // 2
        hbm = pl.BlockSpec(memory_space=pltpu.HBM)
        wide = max(groups * 4, SLOTS * d_ff // d_model * 2)
        out = pl.pallas_call(
            functools.partial(kernel, ring),
            out_shape=(
                jax.ShapeDtypeStruct((tok, d_model), BF16),
                jax.ShapeDtypeStruct((SLOTS, groups, d_model, COLS), BF16),
                jax.ShapeDtypeStruct((SLOTS, blocks, d_ff, COLS), BF16),
            ),
            in_specs=[hbm] * 9,
            out_specs=(hbm, hbm, hbm),
            scratch_shapes=[
                pltpu.VMEM((SLOTS, 2 * tok, d_ff), BF16),
                pltpu.VMEM((2 * tok, d_model), BF16),
                pltpu.VMEM((wide, d_model, COLS), BF16),
                pltpu.VMEM((2 * tok, 128), F32),
                pltpu.VMEM((SLOTS, tok), F32),
                pltpu.VMEM((SLOTS, tok), F32),
                pltpu.VMEM((2, 4, tm, COLS), F32),
                pltpu.VMEM((blocks, 2, tm, COLS), F32),
                pltpu.VMEM((tok, d_model), BF16),
                pltpu.VMEM((2, tm, COLS), BF16),
                pltpu.VMEM((4, d_ff, COLS), BF16),
                pltpu.VMEM((SLOTS, 2 * groups + d_model // 128, 128), F32),
                pltpu.VMEM((SLOTS, 2 * groups + d_model // 128, 128), BF16),
                pltpu.VMEM((128, d_model), BF16),
                pltpu.VMEM(expert_ids.T.shape, jnp.int32),
                pltpu.VMEM((d_model // 128, 128), BF16),
                pltpu.VMEM(router_w.T.shape, BF16),
                pltpu.VMEM(router_b[None].shape, BF16),
                pltpu.VMEM(b_gate_up.shape, BF16),
                pltpu.VMEM(b_down.shape, BF16),
            ],
            compiler_params=pltpu.CompilerParams(collective_id=0, has_side_effects=True, vmem_limit_bytes=67043328),
        )(x_in, expert_ids.T, norm_weight.reshape(-1, 128), router_w.T, router_b[None], w_gate_up, b_gate_up, w_down, b_down)
        chunks = 8
        return pl.pallas_call(
            copy_out,
            out_shape=jax.ShapeDtypeStruct((tok, d_model), BF16),
            in_specs=[hbm],
            out_specs=hbm,
            scratch_shapes=[pltpu.VMEM((chunks, tok // chunks, d_model), BF16), pltpu.SemaphoreType.DMA((chunks,)), pltpu.SemaphoreType.DMA((chunks,))],
            compiler_params=pltpu.CompilerParams(vmem_limit_bytes=60000000),
        )(out[0])

    return jax.shard_map(local_block, mesh=mesh, in_specs=(rows_spec, rows_spec, P(), P(), P(), P('ep', None, None), P('ep', None), P('ep', None, None), P('ep', None)), out_specs=rows_spec, check_vma=False)
```
